32 devices in a mesh: zg: 4 (over x, core), xy: 8 (over z, y).
Axes of the slice: x: 2, y: 2, z: 4, core: 2. Of those that a mesh axis runs over, the one named last changes fastest.
Arguments:
- dipole_field: bfloat16 [2, 3, 16, 512, 256], P(None, None, 'zg', 'xy'), may hold values from -6 to 6
- material: int32 [16, 512, 2], P('zg', 'xy'), may hold values from 0 to 3
- alpha_table: float32 [4, 2, 3, 3], replicated, may hold values from -3 to 3
- green_spectrum: bfloat16 [2, 6, 32, 1024, 512], P(None, None, 'xy', None, 'zg'), may hold values from -6 to 6
- green_scale: float32 [6, 32], P(None, 'xy'), may hold values from 0.5 to 2
Outputs:
- scattered_field: bfloat16 [2, 3, 16, 512, 256], P(None, None, 'zg', 'xy')
The draws below stay inside these ranges and needn't reach their ends.
All inputs are finite; a program needn't handle non-finite values.
Results may differ from the reference program's by a relative error of at most 0.019.
Values may be sent and summed in bfloat16 or wider, within the bound.
No kernel may reach another device: no remote copies, remote signals or barrier semaphores. Data moves between devices by JAX's collectives and lax.ppermute only.
A program may use at most 128 MiB of HBM per device.

```python
import math
import jax
import jax.numpy as jnp
from jax import lax

NZ = 16
NX = 512
NYW = 256
COLB = 128
NMAT = 4
LZ = 32
LX = 1024
LY = 512


def with_ends(values, key, smallest, largest):
    index_at = [jax.random.randint(jax.random.fold_in(key, axis), (), 0, length) for axis, length in enumerate(values.shape)]
    longest = values.shape.index(max(values.shape))
    beside = index_at[:longest] + [(index_at[longest] + 1) % values.shape[longest]] + index_at[longest + 1:]
    return values.at[tuple(index_at)].set(smallest).at[tuple(beside)].set(largest)


def shard_levels(key, shape, cuts, least, largest):
    factor_of = 1.0
    for dim, shards_of in cuts:
        draws = jax.random.uniform(jax.random.fold_in(jax.random.fold_in(key, 6), dim), (shards_of,), jnp.float32, least / len(cuts), largest / len(cuts))
        factor_of = factor_of * jnp.repeat(jnp.exp(draws), shape[dim] // shards_of).reshape((-1,) + (1,) * (len(shape) - 1 - dim))
    return factor_of


def normal_values(key, shape, scale, reach, cuts=(), kind=jnp.bfloat16):
    gain = shard_levels(key, shape, cuts, -0.22, 0.18) if cuts else 1.0
    drawn = jax.random.normal(key, shape, jnp.float32) * scale * gain
    return jnp.minimum(jnp.maximum(drawn, -reach), reach).astype(kind)


def setup_inputs(seed: int = 0) -> dict:
    key_list = jax.random.split(jax.random.key(seed), 6)
    dipole_field = normal_values(key_list[0], (2, 3, NZ, NX, NYW), 1.0, 6.0, ((2, 4), (3, 8)))
    material = with_ends(jax.random.randint(key_list[1], (NZ, NX, NYW // COLB), 0, NMAT), jax.random.fold_in(key_list[1], 1), 0, NMAT - 1).astype(jnp.int32)
    alpha_table = normal_values(key_list[2], (NMAT, 2, 3, 3), 0.5, 3.0, (), jnp.float32)
    green_spectrum = normal_values(key_list[3], (2, 6, LZ, LX, LY), 1.0, 6.0, ((2, 8), (4, 4)))
    green_scale = jnp.clip(jnp.exp(math.log(2.0) - 1.3862944 * jax.random.uniform(key_list[4], (6, LZ), jnp.float32) ** shard_levels(key_list[4], (6, LZ), ((1, 8),), -0.2, 0.2)), 0.5, 2.0)
    return {"dipole_field": dipole_field, "material": material, "alpha_table": alpha_table, "green_spectrum": green_spectrum, "green_scale": green_scale}


pairing = ((0, 3, 4), (3, 1, 5), (4, 5, 2))


def dft_table(count_in, count_out, length, direction):
    source = jnp.arange(count_in, dtype=jnp.int32)[:, None]
    target = jnp.arange(count_out, dtype=jnp.int32)[None, :]
    phases = ((source * target) % length).astype(jnp.float32) * (2.0 * math.pi / length)
    return jnp.cos(phases).astype(jnp.bfloat16), (direction * jnp.sin(phases)).astype(jnp.bfloat16)


def transform(spectrum, tables, form):
    cosine_table, sine_table = tables

    def contract(operand, matrix):
        return jnp.einsum(form, operand.astype(jnp.float32), matrix.astype(jnp.float32))

    out_real = contract(spectrum[0], cosine_table) - contract(spectrum[1], sine_table)
    out_imag = contract(spectrum[0], sine_table) + contract(spectrum[1], cosine_table)
    return jnp.stack([out_real, out_imag])


def moments_of(dipole_field, material, alpha_table):
    counts = alpha_table.shape[0]
    onehot = (material[None] == jnp.arange(counts, dtype=jnp.int32)[:, None, None, None]).astype(jnp.float32)
    tensors = jnp.einsum("mzxb,mrij->rijzxb", onehot, alpha_table.astype(jnp.float32))
    layout = dipole_field.shape
    blocks = material.shape[2]
    values = dipole_field.astype(jnp.float32).reshape(layout[0], layout[1], layout[2], layout[3], blocks, layout[4] // blocks)
    real_part = jnp.einsum("ijzxb,jzxbc->izxbc", tensors[0], values[0]) - jnp.einsum("ijzxb,jzxbc->izxbc", tensors[1], values[1])
    imag_part = jnp.einsum("ijzxb,jzxbc->izxbc", tensors[0], values[1]) + jnp.einsum("ijzxb,jzxbc->izxbc", tensors[1], values[0])
    return jnp.stack([real_part, imag_part]).reshape(layout).astype(jnp.bfloat16)


def spectral(spectrum, green_part, factors):
    weighted = green_part.astype(jnp.float32) * factors
    spectrum_real = spectrum[0].astype(jnp.float32)
    spectrum_imag = spectrum[1].astype(jnp.float32)
    reals = []
    imags = []
    for row_axis in range(3):
        total_real = jnp.zeros(spectrum_real.shape[1:], jnp.float32)
        total_imag = jnp.zeros(spectrum_real.shape[1:], jnp.float32)
        for col_axis in range(3):
            component = pairing[row_axis][col_axis]
            green_real = weighted[0, component]
            green_imag = weighted[1, component]
            total_real = total_real + green_real * spectrum_real[col_axis] - green_imag * spectrum_imag[col_axis]
            total_imag = total_imag + green_real * spectrum_imag[col_axis] + green_imag * spectrum_real[col_axis]
        reals.append(total_real)
        imags.append(total_imag)
    return jnp.stack([jnp.stack(reals), jnp.stack(imags)]).astype(jnp.bfloat16)


def reference(dipole_field, material, alpha_table, green_spectrum, green_scale):
    moments = moments_of(dipole_field, material, alpha_table)
    spectrum_y = transform(moments, dft_table(NYW, LY, LY, -1.0), "czxy,yk->czxk").astype(jnp.bfloat16)
    spectrum_z = transform(spectrum_y, dft_table(NZ, LZ, LZ, -1.0), "czxy,zk->ckxy").astype(jnp.bfloat16)

    def per_plane(members):
        spectrum_plane, green_plane, scale_plane = members
        spectrum_x = transform(spectrum_plane, dft_table(NX, LX, LX, -1.0), "cxy,xk->cky").astype(jnp.bfloat16)
        product = spectral(spectrum_x, green_plane, scale_plane[:, None, None])
        return transform(product, dft_table(LX, NX, LX, 1.0), "cky,kx->cxy").astype(jnp.bfloat16)

    planes = lax.map(per_plane, (jnp.moveaxis(spectrum_z, 2, 0), jnp.moveaxis(green_spectrum, 2, 0), jnp.transpose(green_scale)))
    back_x = jnp.moveaxis(planes, 0, 2)
    back_z = transform(back_x, dft_table(LZ, NZ, LZ, 1.0), "ckxy,kz->czxy").astype(jnp.bfloat16)
    back_y = transform(back_z, dft_table(LY, NYW, LY, 1.0), "czxk,ky->czxy")
    result = dipole_field.astype(jnp.float32) - back_y / float(LX * LY * LZ)
    return result.astype(jnp.bfloat16)
```

```python
import functools
import math

import jax
import jax.numpy as jnp
import numpy as np
from jax import lax
from jax.experimental import pallas as pl
from jax.experimental.pallas import tpu as pltpu
from jax.sharding import PartitionSpec as P

pairing = ((0, 3, 4), (3, 1, 5), (4, 5, 2))

VMEM = pltpu.VMEM
f32 = jnp.float32
bf16 = jnp.bfloat16


def phase(rows, cols, length):
    return (np.outer(rows, cols) % length).astype(np.float64) * (2.0 * math.pi / length)


def table_y(rows_y, length_y, groups):
    ny, nk = rows_y // groups, length_y // groups
    out = np.zeros((groups, groups, 2 * ny, 2 * nk), np.float32)
    for a in range(groups):
        for b in range(groups):
            angle = phase(np.arange(ny) + b * ny, np.arange(nk) + a * nk, length_y)
            cosine, sine = np.cos(angle), -np.sin(angle)
            out[a, b, :ny, :nk] = cosine
            out[a, b, ny:, :nk] = -sine
            out[a, b, :ny, nk:] = sine
            out[a, b, ny:, nk:] = cosine
    return jnp.asarray(out, bf16)


def tables_x(rows_x, length_x):
    half, many = length_x // 2, rows_x // 2
    forward = np.zeros((2, 2 * half, many), np.float32)
    inverse = np.zeros((2, 2 * many, half), np.float32)
    for p in range(2):
        angle = phase(np.arange(half), 2 * np.arange(many) + p, length_x)
        forward[p, :half], forward[p, half:] = np.cos(angle), -np.sin(angle)
        inverse[p, :many], inverse[p, many:] = np.cos(angle).T, np.sin(angle).T
    return jnp.asarray(forward, bf16), jnp.asarray(inverse, bf16)


def parity_order(rows):
    out = np.zeros((rows, rows), np.float32)
    for p in range(2):
        for m in range(rows // 2):
            out[p * (rows // 2) + m, 2 * m + p] = 1.0
    return jnp.asarray(out, bf16)


def swapped(value):
    return pltpu.roll(value, value.shape[-1] // 2, 1)


def times(value, angle, low):
    turn = round(angle / (math.pi / 2.0), 9) % 4
    if turn == 0:
        return value
    if turn == 2:
        return -value
    other = swapped(value)
    if turn in (1, 3):
        s = 1.0 if turn == 1 else -1.0
        return other * jnp.where(low, -s, s)
    c, s = math.cos(angle), math.sin(angle)
    return value * c + other * jnp.where(low, -s, s)


def transform_list(values, sign, low):
    n = len(values)
    if n == 1:
        return values
    even = transform_list(values[0::2], sign, low)
    odd = transform_list(values[1::2], sign, low)
    odd = [times(v, sign * 2.0 * math.pi * k / n, low) for k, v in enumerate(odd)]
    return [e + o for e, o in zip(even, odd)] + [e - o for e, o in zip(even, odd)]


def moments_kernel(where_ref, alpha_ref, field_ref, material_ref, order_ref, *rest, groups, counts):
    outs, scratch = rest[:groups], rest[groups]
    me = where_ref[0]
    _, _, planes, rows, many = field_ref.shape
    blocks = material_ref.shape[2]
    cols = many // blocks
    part = many // groups
    low = lax.broadcasted_iota(jnp.int32, (rows, 2 * part), 1) < part
    for z in range(planes):
        for b in range(blocks):
            mat = jnp.broadcast_to(material_ref[z, :, b : b + 1], (rows, cols))
            masks = [mat == n for n in range(1, counts)]

            def pick(c, i, j):
                value = jnp.full((rows, cols), alpha_ref[((0 * 2 + c) * 3 + i) * 3 + j], f32)
                for n in range(1, counts):
                    value = jnp.where(masks[n - 1], alpha_ref[((n * 2 + c) * 3 + i) * 3 + j], value)
                return value

            reals = [field_ref[0, j, z, :, b * cols : (b + 1) * cols].astype(f32) for j in range(3)]
            imags = [field_ref[1, j, z, :, b * cols : (b + 1) * cols].astype(f32) for j in range(3)]
            for i in range(3):
                re = im = None
                for j in range(3):
                    ar, ai = pick(0, i, j), pick(1, i, j)
                    r = ar * reals[j] - ai * imags[j]
                    m = ar * imags[j] + ai * reals[j]
                    re, im = (r, m) if re is None else (re + r, im + m)
                first = jnp.where(low, re, swapped(im)).astype(bf16)
                second = jnp.where(low, swapped(re), im).astype(bf16)
                for h, v in enumerate((first, second)):
                    v = jnp.dot(order_ref[...], v, preferred_element_type=f32).astype(bf16)
                    scratch[2 * b + h, z, i] = v
    for s in range(groups):
        outs[s][...] = scratch[me ^ s]


def forward_z_kernel(where_ref, *rest, groups, members, held):
    pieces = rest[:groups]
    outs = rest[groups : groups + members * held]
    source, target = rest[groups + members * held :]
    me, at = where_ref[0], where_ref[1]
    planes, comps, rows, lanes = pieces[0].shape
    total = planes * groups
    for s in range(groups):
        source[me ^ s] = pieces[s][...]
    tile = min(16, rows)
    steps = rows // tile
    low = lax.broadcasted_iota(jnp.int32, (tile, lanes), 1) < lanes // 2

    def step(n, carry):
        j = n // steps
        at_row = pl.multiple_of((n % steps) * tile, tile)
        values = [
            source[z // planes, z % planes, j, pl.ds(at_row, tile), :].astype(f32) for z in range(total)
        ]
        even = transform_list(values, -1.0, low)
        for k, v in enumerate(even):
            target[2 * k, j, pl.ds(at_row, tile), :] = v.astype(bf16)
        turned = [times(v, -2.0 * math.pi * z / (2 * total), low) for z, v in enumerate(values)]
        for k, v in enumerate(transform_list(turned, -1.0, low)):
            target[2 * k + 1, j, pl.ds(at_row, tile), :] = v.astype(bf16)
        return carry

    lax.fori_loop(0, comps * steps, step, 0)
    for r in range(held):
        for s in range(members):
            outs[r * members + s][...] = target[(at ^ s) * held + r]


def inverse_z_kernel(where_ref, *rest, groups, members, held):
    pieces = rest[: members * held]
    outs = rest[members * held : members * held + groups]
    source, target = rest[members * held + groups :]
    me, at = where_ref[0], where_ref[1]
    comps, rows, lanes = pieces[0].shape
    total = members * held // 2
    planes = total // groups
    for r in range(held):
        for s in range(members):
            source[(at ^ s) * held + r] = pieces[r * members + s][...]
    tile = min(16, rows)
    steps = rows // tile
    low = lax.broadcasted_iota(jnp.int32, (tile, lanes), 1) < lanes // 2

    def step(n, carry):
        j = n // steps
        at_row = pl.multiple_of((n % steps) * tile, tile)
        values = [source[k, j, pl.ds(at_row, tile), :].astype(f32) for k in range(2 * total)]
        even = transform_list(values[0::2], 1.0, low)
        odd = transform_list(values[1::2], 1.0, low)
        for z in range(total):
            v = even[z] + times(odd[z], 2.0 * math.pi * z / (2 * total), low)
            target[z // planes, z % planes, j, pl.ds(at_row, tile), :] = v.astype(bf16)
        return carry

    lax.fori_loop(0, comps * steps, step, 0)
    for s in range(groups):
        outs[s][...] = target[me ^ s]


def middle_kernel(
    where_ref, scale_ref, tabley_hbm, forward_hbm, inverse_hbm, green_hbm, *rest, plane, groups, members
):
    pieces = rest[:groups]
    outs = rest[groups : 2 * groups]
    tabley, forward, inverse, green, spread, wide, product, sems = rest[2 * groups :]
    me, at = where_ref[0], where_ref[1]
    _, comps, rows, lanes = pieces[0].shape
    half = rows // 2
    copies = [
        pltpu.make_async_copy(tabley_hbm.at[me, me ^ t], tabley.at[pl.ds(t * lanes, lanes)], sems.at[t])
        for t in range(groups)
    ]
    copies.append(pltpu.make_async_copy(forward_hbm, forward, sems.at[groups]))
    copies.append(pltpu.make_async_copy(green_hbm.at[:, :, plane], green, sems.at[groups + 1]))
    copies.append(pltpu.make_async_copy(inverse_hbm, inverse, sems.at[groups + 2]))
    for c in copies:
        c.start()
    for c in copies[:groups]:
        c.wait()
    wave = tabley.shape[1] // 2
    for s in range(members):
        block = jnp.concatenate(
            [pieces[t][s].reshape(comps * rows, lanes) for t in range(groups)], axis=1
        )
        result = jnp.dot(block, tabley[...], preferred_element_type=f32).astype(bf16)
        start = pl.multiple_of((at ^ s) * half, half)
        for j in range(comps):
            for p in range(2):
                spread[j, p, pl.ds(start, half), :] = result[j * rows + p * half : j * rows + (p + 1) * half]
    copies[groups].wait()
    for j in range(comps):
        for p in range(2):
            wide[j, p] = jnp.dot(forward[p], spread[j, p], preferred_element_type=f32)
    copies[groups + 1].wait()
    many = wide.shape[2] // 2
    tile = 16

    def step(n, carry):
        top = pl.multiple_of(n * tile, tile)
        spectra = []
        for j in range(comps):
            re, im = [], []
            for p in range(2):
                c = wide[j, p, pl.ds(top, tile), :]
                s = wide[j, p, pl.ds(many + top, tile), :]
                re.append(c[:, :wave] - s[:, wave:])
                im.append(s[:, :wave] + c[:, wave:])
            spectra.append(((re[0] + re[1], im[0] + im[1]), (re[0] - re[1], im[0] - im[1])))
        totals = []
        for h in range(2):
            weights = [
                tuple(
                    green[c, e, pl.ds(h * many + top, tile), :].astype(f32) * scale_ref[e, plane]
                    for c in range(2)
                )
                for e in range(2 * comps)
            ]
            out = []
            for i in range(comps):
                re = im = None
                for j in range(comps):
                    gr, gi = weights[pairing[i][j]]
                    xr, xi = spectra[j][h]
                    r, m = gr * xr - gi * xi, gr * xi + gi * xr
                    re, im = (r, m) if re is None else (re + r, im + m)
                out.append((re, im))
            totals.append(out)
        for i in range(comps):
            for p in range(2):
                for c in range(2):
                    a, b = totals[0][i][c], totals[1][i][c]
                    product[i, p, pl.ds(top, tile), c * wave : (c + 1) * wave] = (
                        a + b if p == 0 else a - b
                    ).astype(bf16)
        return carry

    lax.fori_loop(0, many // tile, step, 0)
    copies[groups + 2].wait()
    count = inverse.shape[1] // 2
    for i in range(comps):
        for p in range(2):
            both = jnp.dot(inverse[p], product[i, p], preferred_element_type=f32)
            c, s = both[:count], both[count:]
            re = c[:, :wave] - s[:, wave:]
            im = s[:, :wave] + c[:, wave:]
            back = jnp.concatenate([re.astype(bf16), im.astype(bf16)], axis=1)
            share = lax.dot_general(
                back, tabley[...], (((1,), (1,)), ((), ())), preferred_element_type=f32
            ).astype(bf16)
            for b in range(members):
                for t in range(groups):
                    outs[t][at ^ b, i, p * half : (p + 1) * half, :] = share[
                        b * half : (b + 1) * half, t * lanes : (t + 1) * lanes
                    ]


def join_kernel(*refs):
    ins, out = refs[:-1], refs[-1]
    for s, piece in enumerate(ins):
        out[s] = piece[...]


def add_kernel(a, b, out):
    out[...] = (a[...].astype(f32) + b[...].astype(f32)).astype(bf16)


def finish_kernel(a, b, c, *outs):
    for s, out in enumerate(outs):
        out[...] = (a[s].astype(f32) + b[s].astype(f32) + c[s].astype(f32)).astype(bf16)


def result_kernel(where_ref, field_ref, order_ref, *rest, groups, factor):
    pieces, out, scratch = rest[:groups], rest[groups], rest[groups + 1]
    me = where_ref[0]
    _, _, planes, rows, many = field_ref.shape
    part = many // groups
    lanes = 2 * part
    for s in range(groups):
        scratch[me ^ s] = pieces[s][...]
    low = lax.broadcasted_iota(jnp.int32, (rows, lanes), 1) < part
    for z in range(planes):
        for i in range(3):
            for b in range(groups // 2):
                first, second = [
                    lax.dot_general(
                        order_ref[...], scratch[2 * b + h, z, i], (((0,), (0,)), ((), ())),
                        preferred_element_type=f32,
                    )
                    for h in range(2)
                ]
                re = jnp.where(low, first, swapped(second))
                im = jnp.where(low, swapped(first), second)
                for c, v in enumerate((re, im)):
                    field = field_ref[c, i, z, :, b * lanes : (b + 1) * lanes].astype(f32)
                    out[c, i, z, :, b * lanes : (b + 1) * lanes] = (field - v * factor).astype(bf16)


def smem():
    return pl.BlockSpec(memory_space=pltpu.SMEM)


def vmem():
    return pl.BlockSpec(memory_space=pltpu.VMEM)


def hbm():
    return pl.BlockSpec(memory_space=pl.ANY)


def call(kernel, specs, shapes, scratch, flops, args, name):
    many = isinstance(shapes, list)
    return pl.pallas_call(
        kernel,
        in_specs=specs,
        out_specs=[vmem() for _ in shapes] if many else vmem(),
        out_shape=shapes,
        scratch_shapes=scratch,
        compiler_params=pltpu.CompilerParams(vmem_limit_bytes=56 * 1024 * 1024),
        cost_estimate=pl.CostEstimate(flops=int(flops), transcendentals=0, bytes_accessed=1 << 20),
        name=name,
    )(*args)


def on_device(dipole_field, material, alpha_table, green_spectrum, green_scale):
    groups, members = lax.axis_size("zg"), lax.axis_size("xy")
    _, comps, planes, rows, rows_y = dipole_field.shape
    length_y = 2 * rows_y
    rows_x = rows * members
    length_x = 2 * rows_x
    total_z = planes * groups
    length_z = 2 * total_z
    held = length_z // members
    part = rows_y // groups
    lanes = 2 * part
    wave = length_y // groups
    counts = alpha_table.shape[0]
    where = jnp.stack([lax.axis_index("zg"), lax.axis_index("xy")]).astype(jnp.int32)
    tabley = table_y(rows_y, length_y, groups)
    forward, inverse = tables_x(rows_x, length_x)
    order = parity_order(rows)

    def send(value, axis, size, distance):
        return lax.ppermute(value, axis, [(i, i ^ distance) for i in range(size)])

    def exchange(parts, axis):
        return [parts[0]] + [send(parts[s], axis, len(parts), s) for s in range(1, len(parts))]

    def shape(*dims):
        return jax.ShapeDtypeStruct(dims, bf16)

    cycle = 1e6

    parts = call(
        functools.partial(moments_kernel, groups=groups, counts=counts),
        [smem(), smem(), vmem(), vmem(), vmem()],
        [shape(planes, comps, rows, lanes)] * groups,
        [VMEM((groups, planes, comps, rows, lanes), bf16)],
        5e9,
        (where, alpha_table.reshape(-1), dipole_field, material, order),
        "moments",
    )
    parts = exchange(parts, "zg")
    pieces = call(
        functools.partial(forward_z_kernel, groups=groups, members=members, held=held),
        [smem()] + [vmem()] * groups,
        [shape(comps, rows, lanes)] * (members * held),
        [VMEM((groups, planes, comps, rows, lanes), bf16), VMEM((length_z, comps, rows, lanes), bf16)],
        4e9,
        (where, *parts),
        "forward_z",
    )
    full = shape(members, comps, rows, lanes)
    returned = []
    for r in range(held):
        mine = exchange(pieces[r * members : (r + 1) * members], "xy")
        gathered = [call(join_kernel, [vmem()] * members, full, [], 1e9, mine, "join")]
        have = {0: gathered[0]}
        bit = groups // 2
        while bit:
            for t in sorted(have):
                have[t ^ bit] = send(have[t], "zg", groups, bit)
            bit //= 2
        shares = call(
            functools.partial(middle_kernel, plane=r, groups=groups, members=members),
            [smem(), smem(), hbm(), hbm(), hbm(), hbm()] + [vmem()] * groups,
            [full] * groups,
            [
                VMEM((groups * lanes, 2 * wave), bf16),
                VMEM(forward.shape, bf16),
                VMEM(inverse.shape, bf16),
                VMEM((2, 2 * comps, length_x, wave), bf16),
                VMEM((comps, 2, rows_x // 2, 2 * wave), bf16),
                VMEM((comps, 2, length_x, 2 * wave), f32),
                VMEM((comps, 2, length_x // 2, 2 * wave), bf16),
                pltpu.SemaphoreType.DMA((groups + 3,)),
            ],
            8e9,
            (where, green_scale, tabley, forward, inverse, green_spectrum, *[have[t] for t in range(groups)]),
            "middle",
        )
        held_shares = dict(enumerate(shares))
        bit = 1
        while bit < groups // 2:
            moved = {t: send(held_shares[t ^ bit], "zg", groups, bit) for t in held_shares if not t & bit}
            later = {}
            for t in moved:
                if t:
                    later[t] = call(add_kernel, [vmem()] * 2, full, [], 1e9, (held_shares[t], moved[t]), "add")
                else:
                    own = (held_shares[t], moved[t])
            held_shares = later
            bit *= 2
        last = send(held_shares[bit], "zg", groups, bit)
        split = call(
            finish_kernel, [vmem()] * 3, [shape(comps, rows, lanes)] * members, [], 1e9, (*own, last), "finish"
        )
        returned += exchange(split, "xy")
    parts = call(
        functools.partial(inverse_z_kernel, groups=groups, members=members, held=held),
        [smem()] + [vmem()] * (members * held),
        [shape(planes, comps, rows, lanes)] * groups,
        [VMEM((length_z, comps, rows, lanes), bf16), VMEM((groups, planes, comps, rows, lanes), bf16)],
        4e9,
        (where, *returned),
        "inverse_z",
    )
    parts = exchange(parts, "zg")
    return call(
        functools.partial(result_kernel, groups=groups, factor=1.0 / float(length_x * length_y * length_z)),
        [smem(), vmem(), vmem()] + [vmem()] * groups,
        shape(*dipole_field.shape),
        [VMEM((groups, planes, comps, rows, lanes), bf16)],
        3e9,
        (where, dipole_field, order, *parts),
        "result",
    )


def solution(mesh):
    return jax.shard_map(
        on_device,
        mesh=mesh,
        in_specs=(
            P(None, None, "zg", "xy", None),
            P("zg", "xy", None),
            P(),
            P(None, None, "xy", None, "zg"),
            P(None, "xy"),
        ),
        out_specs=P(None, None, "zg", "xy", None),
        check_vma=False,
    )
```

```python
import functools
import math

import jax
import jax.numpy as jnp
import numpy as np
from jax import lax
from jax.experimental import pallas as pl
from jax.experimental.pallas import tpu as pltpu
from jax.sharding import PartitionSpec as P

pairing = ((0, 3, 4), (3, 1, 5), (4, 5, 2))

CHUNK = 2
VMEM = pltpu.VMEM
f32 = jnp.float32
bf16 = jnp.bfloat16


def phase(rows, cols, length):
    return (np.outer(rows, cols) % length).astype(np.float64) * (2.0 * math.pi / length)


def table_y(rows_y, length_y, groups):
    ny, nk = rows_y // groups, length_y // groups
    out = np.zeros((groups, groups, 2 * ny, 2 * nk), np.float32)
    for a in range(groups):
        for b in range(groups):
            angle = phase(np.arange(ny) + b * ny, np.arange(nk) + a * nk, length_y)
            cosine, sine = np.cos(angle), -np.sin(angle)
            out[a, b, :ny, :nk] = cosine
            out[a, b, ny:, :nk] = -sine
            out[a, b, :ny, nk:] = sine
            out[a, b, ny:, nk:] = cosine
    return jnp.asarray(out, bf16)


def tables_x(rows_x, length_x):
    half, many = length_x // 2, rows_x // 2
    forward = np.zeros((2, 2 * half, many), np.float32)
    inverse = np.zeros((2, 2 * many, half), np.float32)
    for p in range(2):
        angle = phase(np.arange(half), 2 * np.arange(many) + p, length_x)
        forward[p, :half], forward[p, half:] = np.cos(angle), -np.sin(angle)
        inverse[p, :many], inverse[p, many:] = np.cos(angle).T, np.sin(angle).T
    return jnp.asarray(forward, bf16), jnp.asarray(inverse, bf16)


def parity_order(rows):
    out = np.zeros((rows, rows), np.float32)
    for p in range(2):
        for m in range(rows // 2):
            out[p * (rows // 2) + m, 2 * m + p] = 1.0
    return jnp.asarray(out, bf16)


def swapped(value):
    return pltpu.roll(value, value.shape[-1] // 2, 1)


def times(value, angle, low):
    turn = round(angle / (math.pi / 2.0), 9) % 4
    if turn == 0:
        return value
    if turn == 2:
        return -value
    other = swapped(value)
    if turn in (1, 3):
        s = 1.0 if turn == 1 else -1.0
        return other * jnp.where(low, -s, s)
    c, s = math.cos(angle), math.sin(angle)
    return value * c + other * jnp.where(low, -s, s)


def transform_list(values, sign, low):
    n = len(values)
    if n == 1:
        return values
    even = transform_list(values[0::2], sign, low)
    odd = transform_list(values[1::2], sign, low)
    odd = [times(v, sign * 2.0 * math.pi * k / n, low) for k, v in enumerate(odd)]
    return [e + o for e, o in zip(even, odd)] + [e - o for e, o in zip(even, odd)]


def moments_kernel(where_ref, alpha_ref, field_ref, material_ref, order_ref, *rest, groups, counts):
    outs, scratch = rest[:groups], rest[groups]
    me = where_ref[0]
    _, _, planes, rows, many = field_ref.shape
    blocks = material_ref.shape[2]
    cols = many // blocks
    part = many // groups
    low = lax.broadcasted_iota(jnp.int32, (rows, 2 * part), 1) < part
    for z in range(planes):
        for b in range(blocks):
            mat = jnp.broadcast_to(material_ref[z, :, b : b + 1], (rows, cols))
            masks = [mat == n for n in range(1, counts)]

            def pick(c, i, j):
                value = jnp.full((rows, cols), alpha_ref[((0 * 2 + c) * 3 + i) * 3 + j], f32)
                for n in range(1, counts):
                    value = jnp.where(masks[n - 1], alpha_ref[((n * 2 + c) * 3 + i) * 3 + j], value)
                return value

            reals = [field_ref[0, j, z, :, b * cols : (b + 1) * cols].astype(f32) for j in range(3)]
            imags = [field_ref[1, j, z, :, b * cols : (b + 1) * cols].astype(f32) for j in range(3)]
            for i in range(3):
                re = im = None
                for j in range(3):
                    ar, ai = pick(0, i, j), pick(1, i, j)
                    r = ar * reals[j] - ai * imags[j]
                    m = ar * imags[j] + ai * reals[j]
                    re, im = (r, m) if re is None else (re + r, im + m)
                first = jnp.where(low, re, swapped(im)).astype(bf16)
                second = jnp.where(low, swapped(re), im).astype(bf16)
                for h, v in enumerate((first, second)):
                    v = jnp.dot(order_ref[...], v, preferred_element_type=f32).astype(bf16)
                    scratch[2 * b + h, z, i] = v
    for s in range(groups):
        outs[s][...] = scratch[me ^ s]


def forward_z_kernel(where_ref, *rest, groups, chunk):
    pieces = rest[:groups]
    outs, source = rest[groups:-1], rest[-1]
    me = where_ref[0]
    held = chunk * len(outs)
    planes, comps, rows, lanes = pieces[0].shape
    total = planes * groups
    for s in range(groups):
        source[me ^ s] = pieces[s][...]
    tile = min(16, rows)
    steps = rows // tile
    low = lax.broadcasted_iota(jnp.int32, (tile, lanes), 1) < lanes // 2

    def step(n, carry):
        j = n // steps
        at_row = pl.multiple_of((n % steps) * tile, tile)
        values = [
            source[z // planes, z % planes, j, pl.ds(at_row, tile), :].astype(f32) for z in range(total)
        ]

        def keep(k, v):
            out = outs[k % held // chunk]
            out[k // held, k % chunk, j, pl.ds(at_row, tile), :] = v.astype(bf16)

        for k, v in enumerate(transform_list(values, -1.0, low)):
            keep(2 * k, v)
        turned = [times(v, -2.0 * math.pi * z / (2 * total), low) for z, v in enumerate(values)]
        for k, v in enumerate(transform_list(turned, -1.0, low)):
            keep(2 * k + 1, v)
        return carry

    lax.fori_loop(0, comps * steps, step, 0)


def inverse_z_kernel(where_ref, *rest, groups, chunks):
    pieces = rest[:chunks]
    outs, target = rest[chunks:-1], rest[-1]
    me = where_ref[0]
    members, chunk, comps, rows, lanes = pieces[0].shape
    held = chunk * chunks
    total = members * held // 2
    planes = total // groups
    tile = min(16, rows)
    steps = rows // tile
    low = lax.broadcasted_iota(jnp.int32, (tile, lanes), 1) < lanes // 2

    def step(n, carry):
        j = n // steps
        at_row = pl.multiple_of((n % steps) * tile, tile)
        values = [
            pieces[k % held // chunk][k // held, k % chunk, j, pl.ds(at_row, tile), :].astype(f32)
            for k in range(2 * total)
        ]
        even = transform_list(values[0::2], 1.0, low)
        odd = transform_list(values[1::2], 1.0, low)
        for z in range(total):
            v = even[z] + times(odd[z], 2.0 * math.pi * z / (2 * total), low)
            target[z // planes, z % planes, j, pl.ds(at_row, tile), :] = v.astype(bf16)
        return carry

    lax.fori_loop(0, comps * steps, step, 0)
    for s in range(groups):
        outs[s][...] = target[me ^ s]


def middle_kernel(
    where_ref, scale_ref, tabley_hbm, forward_hbm, inverse_hbm, green_hbm, *rest, first, chunk, groups, members
):
    pieces = rest[:groups]
    outs = rest[groups : 2 * groups]
    tabley, forward, inverse, green, spread, wide, product, sems = rest[2 * groups :]
    me = where_ref[0]
    _, comps, rows, lanes = pieces[0].shape
    half = rows // 2
    g = pl.program_id(0)
    plane = first + g
    copies = [
        pltpu.make_async_copy(tabley_hbm.at[me, me ^ t], tabley.at[pl.ds(t * lanes, lanes)], sems.at[t])
        for t in range(groups)
    ]
    copies.append(pltpu.make_async_copy(forward_hbm, forward, sems.at[groups]))
    copies.append(pltpu.make_async_copy(inverse_hbm, inverse, sems.at[groups + 1]))
    load = pltpu.make_async_copy(green_hbm.at[:, :, plane], green, sems.at[groups + 2])
    load.start()

    @pl.when(g == 0)
    def _():
        for c in copies:
            c.start()
        for c in copies[:groups]:
            c.wait()

    wave = tabley.shape[1] // 2
    for s in range(members):
        block = jnp.concatenate(
            [pieces[t][s].reshape(comps * rows, lanes) for t in range(groups)], axis=1
        )
        result = jnp.dot(block, tabley[...], preferred_element_type=f32).astype(bf16)
        start = s * half
        for j in range(comps):
            for p in range(2):
                spread[j, p, pl.ds(start, half), :] = result[j * rows + p * half : j * rows + (p + 1) * half]
    @pl.when(g == 0)
    def _():
        copies[groups].wait()

    for j in range(comps):
        for p in range(2):
            wide[j, p] = jnp.dot(forward[p], spread[j, p], preferred_element_type=f32)
    load.wait()
    many = wide.shape[2] // 2
    tile = 16

    def step(n, carry):
        top = pl.multiple_of(n * tile, tile)
        spectra = []
        for j in range(comps):
            re, im = [], []
            for p in range(2):
                c = wide[j, p, pl.ds(top, tile), :]
                s = wide[j, p, pl.ds(many + top, tile), :]
                re.append(c[:, :wave] - s[:, wave:])
                im.append(s[:, :wave] + c[:, wave:])
            spectra.append(((re[0] + re[1], im[0] + im[1]), (re[0] - re[1], im[0] - im[1])))
        totals = []
        for h in range(2):
            weights = [
                tuple(
                    green[c, e, pl.ds(h * many + top, tile), :].astype(f32) * scale_ref[e, plane]
                    for c in range(2)
                )
                for e in range(2 * comps)
            ]
            out = []
            for i in range(comps):
                re = im = None
                for j in range(comps):
                    gr, gi = weights[pairing[i][j]]
                    xr, xi = spectra[j][h]
                    r, m = gr * xr - gi * xi, gr * xi + gi * xr
                    re, im = (r, m) if re is None else (re + r, im + m)
                out.append((re, im))
            totals.append(out)
        for i in range(comps):
            for p in range(2):
                for c in range(2):
                    a, b = totals[0][i][c], totals[1][i][c]
                    product[i, p, pl.ds(top, tile), c * wave : (c + 1) * wave] = (
                        a + b if p == 0 else a - b
                    ).astype(bf16)
        return carry

    lax.fori_loop(0, many // tile, step, 0)
    @pl.when(g == 0)
    def _():
        copies[groups + 1].wait()

    count = inverse.shape[1] // 2
    for i in range(comps):
        for p in range(2):
            both = jnp.dot(inverse[p], product[i, p], preferred_element_type=f32)
            c, s = both[:count], both[count:]
            re = c[:, :wave] - s[:, wave:]
            im = s[:, :wave] + c[:, wave:]
            back = jnp.concatenate([re.astype(bf16), im.astype(bf16)], axis=1)
            share = lax.dot_general(
                back, tabley[...], (((1,), (1,)), ((), ())), preferred_element_type=f32
            ).astype(bf16)
            for b in range(members):
                for t in range(groups):
                    outs[t][b, i, p * half : (p + 1) * half, :] = share[
                        b * half : (b + 1) * half, t * lanes : (t + 1) * lanes
                    ]


def result_kernel(where_ref, field_ref, order_ref, *rest, groups, factor):
    pieces, out, scratch = rest[:groups], rest[groups], rest[groups + 1]
    me = where_ref[0]
    _, _, planes, rows, many = field_ref.shape
    part = many // groups
    lanes = 2 * part
    for s in range(groups):
        scratch[me ^ s] = pieces[s][...]
    low = lax.broadcasted_iota(jnp.int32, (rows, lanes), 1) < part
    for z in range(planes):
        for i in range(3):
            for b in range(groups // 2):
                first, second = [
                    lax.dot_general(
                        order_ref[...], scratch[2 * b + h, z, i], (((0,), (0,)), ((), ())),
                        preferred_element_type=f32,
                    )
                    for h in range(2)
                ]
                re = jnp.where(low, first, swapped(second))
                im = jnp.where(low, swapped(first), second)
                for c, v in enumerate((re, im)):
                    field = field_ref[c, i, z, :, b * lanes : (b + 1) * lanes].astype(f32)
                    out[c, i, z, :, b * lanes : (b + 1) * lanes] = (field - v * factor).astype(bf16)


def smem():
    return pl.BlockSpec(memory_space=pltpu.SMEM)


def vmem():
    return pl.BlockSpec(memory_space=pltpu.VMEM)


def hbm():
    return pl.BlockSpec(memory_space=pl.ANY)


def call(kernel, specs, shapes, scratch, flops, args, name, grid=(), out_spec=None):
    many = isinstance(shapes, list)
    return pl.pallas_call(
        kernel,
        grid=grid,
        in_specs=specs,
        out_specs=[out_spec or vmem() for _ in shapes] if many else vmem(),
        out_shape=shapes,
        scratch_shapes=scratch,
        compiler_params=pltpu.CompilerParams(vmem_limit_bytes=56 * 1024 * 1024),
        cost_estimate=pl.CostEstimate(flops=int(flops), transcendentals=0, bytes_accessed=1 << 20),
        name=name,
    )(*args)


def on_device(dipole_field, material, alpha_table, green_spectrum, green_scale):
    groups, members = lax.axis_size("zg"), lax.axis_size("xy")
    _, comps, planes, rows, rows_y = dipole_field.shape
    length_y = 2 * rows_y
    rows_x = rows * members
    length_x = 2 * rows_x
    total_z = planes * groups
    length_z = 2 * total_z
    held = length_z // members
    part = rows_y // groups
    lanes = 2 * part
    wave = length_y // groups
    counts = alpha_table.shape[0]
    where = jnp.stack([lax.axis_index("zg"), lax.axis_index("xy")]).astype(jnp.int32)
    tabley = table_y(rows_y, length_y, groups)
    forward, inverse = tables_x(rows_x, length_x)
    order = parity_order(rows)

    def send(value, axis, size, distance):
        return lax.ppermute(value, axis, [(i, i ^ distance) for i in range(size)])

    def exchange(parts, axis):
        return [parts[0]] + [send(parts[s], axis, len(parts), s) for s in range(1, len(parts))]

    def shape(*dims):
        return jax.ShapeDtypeStruct(dims, bf16)

    cycle = 1e6

    parts = call(
        functools.partial(moments_kernel, groups=groups, counts=counts),
        [smem(), smem(), vmem(), vmem(), vmem()],
        [shape(planes, comps, rows, lanes)] * groups,
        [VMEM((groups, planes, comps, rows, lanes), bf16)],
        5e9,
        (where, alpha_table.reshape(-1), dipole_field, material, order),
        "moments",
    )
    parts = exchange(parts, "zg")
    chunk = min(CHUNK, held)
    chunks = held // chunk
    full = shape(members, chunk, comps, rows, lanes)
    pieces = call(
        functools.partial(forward_z_kernel, groups=groups, chunk=chunk),
        [smem()] + [vmem()] * groups,
        [full] * chunks,
        [VMEM((groups, planes, comps, rows, lanes), bf16)],
        4e9,
        (where, *parts),
        "forward_z",
    )
    block = pl.BlockSpec((members, None, comps, rows, lanes), lambda g: (0, g, 0, 0, 0))

    def after(value, *others):
        return lax.optimization_barrier((value, *others))[0] if others else value

    def across(value):
        return lax.all_to_all(value, "xy", 0, 0, tiled=True)

    def gather(value):
        have = {0: value}
        bit = groups // 2
        while bit:
            for t in sorted(have):
                have[t ^ bit] = send(have[t], "zg", groups, bit)
            bit //= 2
        return [have[t] for t in range(groups)]

    def middle(r, have):
        return call(
            functools.partial(middle_kernel, first=r * chunk, chunk=chunk, groups=groups, members=members),
            [smem(), smem(), hbm(), hbm(), hbm(), hbm()] + [block] * groups,
            [full] * groups,
            [
                VMEM((groups * lanes, 2 * wave), bf16),
                VMEM(forward.shape, bf16),
                VMEM(inverse.shape, bf16),
                VMEM((2, 2 * comps, length_x, wave), bf16),
                VMEM((comps, 2, rows_x // 2, 2 * wave), bf16),
                VMEM((comps, 2, length_x, 2 * wave), f32),
                VMEM((comps, 2, length_x // 2, 2 * wave), bf16),
                pltpu.SemaphoreType.DMA((groups + 3,)),
            ],
            8e9 * chunk,
            (where, green_scale, tabley, forward, inverse, green_spectrum, *have),
            "middle",
            grid=(chunk,),
            out_spec=block,
        )

    def reduce(shares):
        shares = dict(enumerate(shares))
        bit = 1
        while bit < groups // 2:
            moved = {t: send(shares[t ^ bit], "zg", groups, bit) for t in shares if not t & bit}
            shares = {
                t: (shares[t].astype(f32) + moved[t].astype(f32)).astype(bf16) if t else (shares[t], moved[t])
                for t in moved
            }
            bit *= 2
        own, moved = shares[0]
        last = send(shares[bit], "zg", groups, bit)
        return (own.astype(f32) + moved.astype(f32) + last.astype(f32)).astype(bf16)

    arrived, shared, totals = [], [], []
    for r in range(chunks):
        value = after(pieces[r], *arrived[-1:])
        arrived.append(across(value))
    ready = []
    for r in range(chunks):
        have = gather(after(arrived[r], *(shared[r - 2][:1] if r >= 2 else [])))
        ready.append(have)
        if r + 1 < chunks:
            have = [after(have[0], arrived[r + 1])] + have[1:]
        shared.append(middle(r, have))
    returned = []
    for r in range(chunks):
        returned.append(across(after(reduce(shared[r]), *returned[-1:])))
    parts = call(
        functools.partial(inverse_z_kernel, groups=groups, chunks=chunks),
        [smem()] + [vmem()] * chunks,
        [shape(planes, comps, rows, lanes)] * groups,
        [VMEM((groups, planes, comps, rows, lanes), bf16)],
        4e9,
        (where, *returned),
        "inverse_z",
    )
    parts = exchange(parts, "zg")
    return call(
        functools.partial(result_kernel, groups=groups, factor=1.0 / float(length_x * length_y * length_z)),
        [smem(), vmem(), vmem()] + [vmem()] * groups,
        shape(*dipole_field.shape),
        [VMEM((groups, planes, comps, rows, lanes), bf16)],
        3e9,
        (where, dipole_field, order, *parts),
        "result",
    )


def solution(mesh):
    return jax.shard_map(
        on_device,
        mesh=mesh,
        in_specs=(
            P(None, None, "zg", "xy", None),
            P("zg", "xy", None),
            P(),
            P(None, None, "xy", None, "zg"),
            P(None, "xy"),
        ),
        out_specs=P(None, None, "zg", "xy", None),
        check_vma=False,
    )
```

```python
import functools
import math

import jax
import jax.numpy as jnp
import numpy as np
from jax import lax
from jax.experimental import pallas as pl
from jax.experimental.pallas import tpu as pltpu
from jax.sharding import PartitionSpec as P

pairing = ((0, 3, 4), (3, 1, 5), (4, 5, 2))

VMEM = pltpu.VMEM
f32 = jnp.float32
bf16 = jnp.bfloat16


def phase(rows, cols, length):
    return (np.outer(rows, cols) % length).astype(np.float64) * (2.0 * math.pi / length)


def table_y(rows_y, length_y, groups):
    ny, nk = rows_y // groups, length_y // groups
    out = np.zeros((groups, groups, 2 * ny, 2 * nk), np.float32)
    for a in range(groups):
        for b in range(groups):
            angle = phase(np.arange(ny) + b * ny, np.arange(nk) + a * nk, length_y)
            cosine, sine = np.cos(angle), -np.sin(angle)
            out[a, b, :ny, :nk] = cosine
            out[a, b, ny:, :nk] = -sine
            out[a, b, :ny, nk:] = sine
            out[a, b, ny:, nk:] = cosine
    return jnp.asarray(out, bf16)


def tables_x(rows_x, length_x):
    half, many = length_x // 2, rows_x // 2
    forward = np.zeros((2, 2 * half, many), np.float32)
    inverse = np.zeros((2, 2 * many, half), np.float32)
    for p in range(2):
        angle = phase(np.arange(half), 2 * np.arange(many) + p, length_x)
        forward[p, :half], forward[p, half:] = np.cos(angle), -np.sin(angle)
        inverse[p, :many], inverse[p, many:] = np.cos(angle).T, np.sin(angle).T
    return jnp.asarray(forward, bf16), jnp.asarray(inverse, bf16)


def parity_order(rows):
    out = np.zeros((rows, rows), np.float32)
    for p in range(2):
        for m in range(rows // 2):
            out[p * (rows // 2) + m, 2 * m + p] = 1.0
    return jnp.asarray(out, bf16)


def swapped(value):
    return pltpu.roll(value, value.shape[-1] // 2, 1)


def times(value, angle, low):
    turn = round(angle / (math.pi / 2.0), 9) % 4
    if turn == 0:
        return value
    if turn == 2:
        return -value
    other = swapped(value)
    if turn in (1, 3):
        s = 1.0 if turn == 1 else -1.0
        return other * jnp.where(low, -s, s)
    c, s = math.cos(angle), math.sin(angle)
    return value * c + other * jnp.where(low, -s, s)


def transform_list(values, sign, low):
    n = len(values)
    if n == 1:
        return values
    even = transform_list(values[0::2], sign, low)
    odd = transform_list(values[1::2], sign, low)
    odd = [times(v, sign * 2.0 * math.pi * k / n, low) for k, v in enumerate(odd)]
    return [e + o for e, o in zip(even, odd)] + [e - o for e, o in zip(even, odd)]


def moments_kernel(alpha_ref, field_ref, material_ref, order_ref, *rest, groups, counts):
    outs, scratch = rest[:groups], rest[groups]
    me = lax.axis_index("zg")
    _, comps, rows, many = field_ref.shape
    blocks = material_ref.shape[0]
    cols = many // blocks
    part = many // groups
    per = cols // part
    low = lax.broadcasted_iota(jnp.int32, (rows, 2 * part), 1) < part
    diagonal = lax.broadcasted_iota(jnp.int32, (rows, rows), 0) == lax.broadcasted_iota(jnp.int32, (rows, rows), 1)
    for b in range(blocks):
        along = jnp.broadcast_to(material_ref[b : b + 1, :].astype(f32), (rows, rows))
        mat = jnp.sum(jnp.where(diagonal, along, 0.0), axis=1, keepdims=True)
        mat = jnp.broadcast_to(mat, (rows, cols))
        masks = [mat == float(n) for n in range(1, counts)]

        def pick(c, i, j):
            value = jnp.full((rows, cols), alpha_ref[i, j, c, 0], f32)
            for n in range(1, counts):
                value = jnp.where(masks[n - 1], alpha_ref[i, j, c, n], value)
            return value

        reals = [field_ref[0, j, :, b * cols : (b + 1) * cols].astype(f32) for j in range(comps)]
        imags = [field_ref[1, j, :, b * cols : (b + 1) * cols].astype(f32) for j in range(comps)]
        for i in range(comps):
            re = im = None
            for j in range(comps):
                ar, ai = pick(0, i, j), pick(1, i, j)
                r = ar * reals[j] - ai * imags[j]
                m = ar * imags[j] + ai * reals[j]
                re, im = (r, m) if re is None else (re + r, im + m)
            first = jnp.where(low, re, swapped(im)).astype(bf16)
            second = jnp.where(low, swapped(re), im).astype(bf16)
            for h, v in enumerate((first, second)):
                scratch[per * b + h, i] = jnp.dot(order_ref[...], v, preferred_element_type=f32).astype(bf16)
    for s in range(groups):
        outs[s][...] = scratch[me ^ s]


def forward_z_kernel(*rest, groups, places):
    pieces = rest[:groups]
    outs, source = rest[groups:-1], rest[-1]
    me = lax.axis_index("zg")
    held = len(places)
    planes, rows, lanes = pieces[0].shape
    total = planes * groups
    for s in range(groups):
        source[me ^ s] = pieces[s][...]
    tile = min(16, rows)
    low = lax.broadcasted_iota(jnp.int32, (tile, lanes), 1) < lanes // 2

    def step(n, carry):
        top = pl.multiple_of(n * tile, tile)

        def values():
            return [source[z // planes, z % planes, pl.ds(top, tile), :].astype(f32) for z in range(total)]

        def keep(k, v):
            chunk, place = places[k % held]
            outs[chunk][k // held, place, pl.ds(top, tile), :] = v.astype(bf16)

        for k, v in enumerate(transform_list(values(), -1.0, low)):
            keep(2 * k, v)
        turned = [times(v, -2.0 * math.pi * z / (2 * total), low) for z, v in enumerate(values())]
        for k, v in enumerate(transform_list(turned, -1.0, low)):
            keep(2 * k + 1, v)
        return carry

    lax.fori_loop(0, rows // tile, step, 0)


def inverse_z_kernel(*rest, groups, places, chunks):
    pieces = rest[:chunks]
    outs, target = rest[chunks:-1], rest[-1]
    me = lax.axis_index("zg")
    members, _, rows, lanes = pieces[0].shape
    held = len(places)
    total = members * held // 2
    planes = total // groups
    tile = min(16, rows)
    low = lax.broadcasted_iota(jnp.int32, (tile, lanes), 1) < lanes // 2

    def step(n, carry):
        top = pl.multiple_of(n * tile, tile)

        def value(k):
            chunk, place = places[k % held]
            return pieces[chunk][k // held, place, pl.ds(top, tile), :].astype(f32)

        even = transform_list([value(k) for k in range(0, 2 * total, 2)], 1.0, low)
        odd = transform_list([value(k) for k in range(1, 2 * total, 2)], 1.0, low)
        for z in range(total):
            v = even[z] + times(odd[z], 2.0 * math.pi * z / (2 * total), low)
            target[z // planes, z % planes, pl.ds(top, tile), :] = v.astype(bf16)
        return carry

    lax.fori_loop(0, rows // tile, step, 0)
    for s in range(groups):
        outs[s][...] = target[me ^ s]


def middle_kernel(
    scale_ref, tabley_hbm, forward_hbm, inverse_hbm, green_hbm, *rest, first, chunk, groups, members
):
    pieces = rest[:groups]
    outs = rest[groups : 2 * groups]
    tabley, forward, inverse, green, spread, wide, product, sems = rest[2 * groups :]
    me = lax.axis_index("zg")
    _, comps, rows, lanes = pieces[0].shape
    half = rows // 2
    g = pl.program_id(0)
    plane = first + g
    copies = [
        pltpu.make_async_copy(tabley_hbm.at[me, me ^ t], tabley.at[pl.ds(t * lanes, lanes)], sems.at[t])
        for t in range(groups)
    ]
    copies.append(pltpu.make_async_copy(forward_hbm, forward, sems.at[groups]))
    copies.append(pltpu.make_async_copy(inverse_hbm, inverse, sems.at[groups + 1]))
    load = pltpu.make_async_copy(green_hbm.at[:, :, plane], green, sems.at[groups + 2])
    load.start()

    @pl.when(g == 0)
    def _():
        for c in copies:
            c.start()
        for c in copies[:groups]:
            c.wait()

    wave = tabley.shape[1] // 2
    for s in range(members):
        block = jnp.concatenate(
            [pieces[t][s].reshape(comps * rows, lanes) for t in range(groups)], axis=1
        )
        result = jnp.dot(block, tabley[...], preferred_element_type=f32).astype(bf16)
        start = s * half
        for j in range(comps):
            for p in range(2):
                spread[j, p, pl.ds(start, half), :] = result[j * rows + p * half : j * rows + (p + 1) * half]
    @pl.when(g == 0)
    def _():
        copies[groups].wait()

    for j in range(comps):
        for p in range(2):
            wide[j, p] = jnp.dot(forward[p], spread[j, p], preferred_element_type=f32)
    load.wait()
    many = wide.shape[2] // 2
    tile = 16

    def step(n, carry):
        top = pl.multiple_of(n * tile, tile)
        spectra = []
        for j in range(comps):
            re, im = [], []
            for p in range(2):
                c = wide[j, p, pl.ds(top, tile), :]
                s = wide[j, p, pl.ds(many + top, tile), :]
                re.append(c[:, :wave] - s[:, wave:])
                im.append(s[:, :wave] + c[:, wave:])
            spectra.append(((re[0] + re[1], im[0] + im[1]), (re[0] - re[1], im[0] - im[1])))
        totals = []
        for h in range(2):
            weights = [
                tuple(
                    green[c, e, pl.ds(h * many + top, tile), :].astype(f32) * scale_ref[plane, e]
                    for c in range(2)
                )
                for e in range(2 * comps)
            ]
            out = []
            for i in range(comps):
                re = im = None
                for j in range(comps):
                    gr, gi = weights[pairing[i][j]]
                    xr, xi = spectra[j][h]
                    r, m = gr * xr - gi * xi, gr * xi + gi * xr
                    re, im = (r, m) if re is None else (re + r, im + m)
                out.append((re, im))
            totals.append(out)
        for i in range(comps):
            for p in range(2):
                for c in range(2):
                    a, b = totals[0][i][c], totals[1][i][c]
                    product[i, p, pl.ds(top, tile), c * wave : (c + 1) * wave] = (
                        a + b if p == 0 else a - b
                    ).astype(bf16)
        return carry

    lax.fori_loop(0, many // tile, step, 0)
    @pl.when(g == 0)
    def _():
        copies[groups + 1].wait()

    count = inverse.shape[1] // 2
    for i in range(comps):
        for p in range(2):
            both = jnp.dot(inverse[p], product[i, p], preferred_element_type=f32)
            c, s = both[:count], both[count:]
            re = c[:, :wave] - s[:, wave:]
            im = s[:, :wave] + c[:, wave:]
            back = jnp.concatenate([re.astype(bf16), im.astype(bf16)], axis=1)
            share = lax.dot_general(
                back, tabley[...], (((1,), (1,)), ((), ())), preferred_element_type=f32
            ).astype(bf16)
            for b in range(members):
                for t in range(groups):
                    outs[t][b, i, p * half : (p + 1) * half, :] = share[
                        b * half : (b + 1) * half, t * lanes : (t + 1) * lanes
                    ]


def result_kernel(field_ref, order_ref, *rest, groups, factor):
    pieces, out, scratch = rest[:groups], rest[groups], rest[groups + 1]
    me = lax.axis_index("zg")
    _, comps, planes, rows, many = field_ref.shape
    part = many // groups
    lanes = 2 * part
    for s in range(groups):
        scratch[me ^ s] = pieces[s][...]
    low = lax.broadcasted_iota(jnp.int32, (rows, lanes), 1) < part
    for z in range(planes):
        for i in range(comps):
            for b in range(groups // 2):
                first, second = [
                    lax.dot_general(
                        order_ref[...], scratch[2 * b + h, z, i], (((0,), (0,)), ((), ())),
                        preferred_element_type=f32,
                    )
                    for h in range(2)
                ]
                re = jnp.where(low, first, swapped(second))
                im = jnp.where(low, swapped(first), second)
                for c, v in enumerate((re, im)):
                    field = field_ref[c, i, z, :, b * lanes : (b + 1) * lanes].astype(f32)
                    out[c, i, z, :, b * lanes : (b + 1) * lanes] = (field - v * factor).astype(bf16)


def smem():
    return pl.BlockSpec(memory_space=pltpu.SMEM)


def vmem():
    return pl.BlockSpec(memory_space=pltpu.VMEM)


def hbm():
    return pl.BlockSpec(memory_space=pl.ANY)


def call(kernel, specs, shapes, scratch, flops, args, name, grid=(), out_spec=None):
    many = isinstance(shapes, list)
    return pl.pallas_call(
        kernel,
        grid=grid,
        in_specs=specs,
        out_specs=(out_spec if isinstance(out_spec, list) else [out_spec] * len(shapes)) if many else out_spec,
        out_shape=shapes,
        scratch_shapes=scratch,
        compiler_params=pltpu.CompilerParams(vmem_limit_bytes=56 * 1024 * 1024),
        cost_estimate=pl.CostEstimate(flops=int(flops), transcendentals=0, bytes_accessed=1 << 20),
        name=name,
    )(*args)


def chunk_sizes(held):
    edge = max(1, held // 2)
    return [edge] * (held // edge)


def on_device(dipole_field, material, alpha_table, green_spectrum, green_scale):
    groups, members = lax.axis_size("zg"), lax.axis_size("xy")
    _, comps, planes, rows, rows_y = dipole_field.shape
    length_y = 2 * rows_y
    rows_x = rows * members
    length_x = 2 * rows_x
    total_z = planes * groups
    length_z = 2 * total_z
    held = length_z // members
    part = rows_y // groups
    lanes = 2 * part
    wave = length_y // groups
    counts = alpha_table.shape[0]
    tabley = table_y(rows_y, length_y, groups)
    forward, inverse = tables_x(rows_x, length_x)
    order = parity_order(rows)

    def send(value, axis, size, distance):
        return lax.ppermute(value, axis, [(i, i ^ distance) for i in range(size)])

    def exchange(parts, axis):
        return [parts[0]] + [send(parts[s], axis, len(parts), s) for s in range(1, len(parts))]

    def shape(*dims):
        return jax.ShapeDtypeStruct(dims, bf16)

    plane_block = pl.BlockSpec((2, comps, None, rows, rows_y), lambda z: (0, 0, z, 0, 0))
    part_block = pl.BlockSpec((None, comps, rows, lanes), lambda z: (z, 0, 0, 0))
    blocks = material.shape[2]
    parts = call(
        functools.partial(moments_kernel, groups=groups, counts=counts),
        [smem(), plane_block, pl.BlockSpec((None, blocks, rows), lambda z: (z, 0, 0)), vmem()],
        [shape(planes, comps, rows, lanes)] * groups,
        [VMEM((groups, comps, rows, lanes), bf16)],
        5e9,
        (jnp.transpose(alpha_table, (2, 3, 1, 0)), dipole_field, jnp.transpose(material, (0, 2, 1)), order),
        "moments",
        grid=(planes,),
        out_spec=part_block,
    )
    parts = exchange(parts, "zg")
    sizes = chunk_sizes(held)
    chunks = len(sizes)
    places = [(c, n) for c, size in enumerate(sizes) for n in range(size)]
    fulls = [shape(members, size, comps, rows, lanes) for size in sizes]
    comp_block = pl.BlockSpec((planes, None, rows, lanes), lambda j: (0, j, 0, 0))
    chunk_blocks = [
        pl.BlockSpec((members, size, None, rows, lanes), lambda j: (0, 0, j, 0, 0)) for size in sizes
    ]
    pieces = call(
        functools.partial(forward_z_kernel, groups=groups, places=places),
        [comp_block] * groups,
        fulls,
        [VMEM((groups, planes, rows, lanes), bf16)],
        4e9,
        tuple(parts),
        "forward_z",
        grid=(comps,),
        out_spec=chunk_blocks,
    )
    block = pl.BlockSpec((members, None, comps, rows, lanes), lambda g: (0, g, 0, 0, 0))

    def after(value, *others):
        return lax.optimization_barrier((value, *others))[0] if others else value

    def across(value):
        return lax.all_to_all(value, "xy", 0, 0, tiled=True)

    def gather(value):
        have = {0: value}
        bit = groups // 2
        while bit:
            for t in sorted(have):
                have[t ^ bit] = send(have[t], "zg", groups, bit)
            bit //= 2
        return [have[t] for t in range(groups)]

    def middle(r, have):
        return call(
            functools.partial(
                middle_kernel, first=sum(sizes[:r]), chunk=sizes[r], groups=groups, members=members
            ),
            [smem(), hbm(), hbm(), hbm(), hbm()] + [block] * groups,
            [fulls[r]] * groups,
            [
                VMEM((groups * lanes, 2 * wave), bf16),
                VMEM(forward.shape, bf16),
                VMEM(inverse.shape, bf16),
                VMEM((2, 2 * comps, length_x, wave), bf16),
                VMEM((comps, 2, rows_x // 2, 2 * wave), bf16),
                VMEM((comps, 2, length_x, 2 * wave), f32),
                VMEM((comps, 2, length_x // 2, 2 * wave), bf16),
                pltpu.SemaphoreType.DMA((groups + 3,)),
            ],
            8e9 * sizes[r],
            (jnp.transpose(green_scale), tabley, forward, inverse, green_spectrum, *have),
            "middle",
            grid=(sizes[r],),
            out_spec=block,
        )

    def reduce(shares):
        shares = dict(enumerate(shares))
        bit = 1
        while bit < groups // 2:
            moved = {t: send(shares[t ^ bit], "zg", groups, bit) for t in shares if not t & bit}
            shares = {
                t: (shares[t].astype(f32) + moved[t].astype(f32)).astype(bf16) if t else (shares[t], moved[t])
                for t in moved
            }
            bit *= 2
        own, moved = shares[0]
        last = send(shares[bit], "zg", groups, bit)
        return (own.astype(f32) + moved.astype(f32) + last.astype(f32)).astype(bf16)

    arrived, shared, totals = [], [], []
    for r in range(chunks):
        value = after(pieces[r], *arrived[-1:])
        arrived.append(across(value))
    ready = []
    for r in range(chunks):
        have = gather(after(arrived[r], *(shared[r - 2][:1] if r >= 2 else [])))
        ready.append(have)
        if r + 1 < chunks:
            have = [after(have[0], arrived[r + 1])] + have[1:]
        shared.append(middle(r, have))
    returned = []
    for r in range(chunks):
        returned.append(across(after(reduce(shared[r]), *returned[-1:])))
    parts = call(
        functools.partial(inverse_z_kernel, groups=groups, places=places, chunks=chunks),
        chunk_blocks,
        [shape(planes, comps, rows, lanes)] * groups,
        [VMEM((groups, planes, rows, lanes), bf16)],
        4e9,
        tuple(returned),
        "inverse_z",
        grid=(comps,),
        out_spec=comp_block,
    )
    parts = exchange(parts, "zg")
    return call(
        functools.partial(result_kernel, groups=groups, factor=1.0 / float(length_x * length_y * length_z)),
        [vmem()] * (2 + groups),
        shape(*dipole_field.shape),
        [VMEM((groups, planes, comps, rows, lanes), bf16)],
        3e9,
        (dipole_field, order, *parts),
        "result",
        out_spec=vmem(),
    )


def solution(mesh):
    return jax.shard_map(
        on_device,
        mesh=mesh,
        in_specs=(
            P(None, None, "zg", "xy", None),
            P("zg", "xy", None),
            P(),
            P(None, None, "xy", None, "zg"),
            P(None, "xy"),
        ),
        out_specs=P(None, None, "zg", "xy", None),
        check_vma=False,
    )
```

```python
import functools
import math

import jax
import jax.numpy as jnp
import numpy as np
from jax import lax
from jax.experimental import pallas as pl
from jax.experimental.pallas import tpu as pltpu
from jax.sharding import PartitionSpec as P

pairing = ((0, 3, 4), (3, 1, 5), (4, 5, 2))

VMEM = pltpu.VMEM
f32 = jnp.float32
bf16 = jnp.bfloat16


def phase(rows, cols, length):
    return (np.outer(rows, cols) % length).astype(np.float64) * (2.0 * math.pi / length)


def table_y(rows_y, length_y, groups):
    ny, nk = rows_y // groups, length_y // groups
    out = np.zeros((groups, groups, 2 * ny, 2 * nk), np.float32)
    for a in range(groups):
        for b in range(groups):
            angle = phase(np.arange(ny) + b * ny, np.arange(nk) + a * nk, length_y)
            cosine, sine = np.cos(angle), -np.sin(angle)
            out[a, b, :ny, :nk] = cosine
            out[a, b, ny:, :nk] = -sine
            out[a, b, :ny, nk:] = sine
            out[a, b, ny:, nk:] = cosine
    return jnp.asarray(out, bf16)


def tables_x(rows_x, length_x):
    half, many = length_x // 2, rows_x // 2
    forward = np.zeros((2, 2 * half, many), np.float32)
    inverse = np.zeros((2, 2 * many, half), np.float32)
    for p in range(2):
        angle = phase(np.arange(half), 2 * np.arange(many) + p, length_x)
        forward[p, :half], forward[p, half:] = np.cos(angle), -np.sin(angle)
        inverse[p, :many], inverse[p, many:] = np.cos(angle).T, np.sin(angle).T
    return jnp.asarray(forward, bf16), jnp.asarray(inverse, bf16)


def parity_order(rows):
    out = np.zeros((rows, rows), np.float32)
    for p in range(2):
        for m in range(rows // 2):
            out[p * (rows // 2) + m, 2 * m + p] = 1.0
    return jnp.asarray(out, bf16)


def swapped(value):
    return pltpu.roll(value, value.shape[-1] // 2, 1)


def opened(value, low):
    half = value.shape[0] // 2
    a, b = value[:half], value[half:]
    return jnp.where(low, a, swapped(b)), jnp.where(low, swapped(a), b)


def closed(pair, low):
    re, im = pair
    return jnp.concatenate([jnp.where(low, re, swapped(im)), jnp.where(low, swapped(re), im)], axis=0)


def plus(a, b):
    return a[0] + b[0], a[1] + b[1]


def minus(a, b):
    return a[0] - b[0], a[1] - b[1]


def times(pair, angle):
    re, im = pair
    turn = round(angle / (math.pi / 2.0), 9) % 4
    if turn in (0, 1, 2, 3):
        return ((re, im), (-im, re), (-re, -im), (im, -re))[int(turn)]
    c, s = math.cos(angle), math.sin(angle)
    return re * c - im * s, re * s + im * c


def transform_list(values, sign):
    n = len(values)
    if n == 1:
        return values
    even = transform_list(values[0::2], sign)
    odd = transform_list(values[1::2], sign)
    odd = [times(v, sign * 2.0 * math.pi * k / n) for k, v in enumerate(odd)]
    return [plus(e, o) for e, o in zip(even, odd)] + [minus(e, o) for e, o in zip(even, odd)]


def moments_kernel(alpha_ref, field_ref, material_ref, order_ref, *rest, groups, counts):
    outs, scratch = rest[:groups], rest[groups]
    me = lax.axis_index("zg")
    _, comps, rows, many = field_ref.shape
    blocks = material_ref.shape[0]
    cols = many // blocks
    part = many // groups
    per = cols // part
    low = lax.broadcasted_iota(jnp.int32, (rows, 2 * part), 1) < part
    diagonal = lax.broadcasted_iota(jnp.int32, (rows, rows), 0) == lax.broadcasted_iota(jnp.int32, (rows, rows), 1)
    for b in range(blocks):
        along = jnp.broadcast_to(material_ref[b : b + 1, :].astype(f32), (rows, rows))
        mat = jnp.sum(jnp.where(diagonal, along, 0.0), axis=1, keepdims=True)
        mat = jnp.broadcast_to(mat, (rows, cols))
        masks = [mat == float(n) for n in range(1, counts)]

        def pick(c, i, j):
            value = jnp.full((rows, cols), alpha_ref[i, j, c, 0], f32)
            for n in range(1, counts):
                value = jnp.where(masks[n - 1], alpha_ref[i, j, c, n], value)
            return value

        reals = [field_ref[0, j, :, b * cols : (b + 1) * cols].astype(f32) for j in range(comps)]
        imags = [field_ref[1, j, :, b * cols : (b + 1) * cols].astype(f32) for j in range(comps)]
        for i in range(comps):
            re = im = None
            for j in range(comps):
                ar, ai = pick(0, i, j), pick(1, i, j)
                r = ar * reals[j] - ai * imags[j]
                m = ar * imags[j] + ai * reals[j]
                re, im = (r, m) if re is None else (re + r, im + m)
            first = jnp.where(low, re, swapped(im)).astype(bf16)
            second = jnp.where(low, swapped(re), im).astype(bf16)
            for h, v in enumerate((first, second)):
                scratch[per * b + h, i] = jnp.dot(order_ref[...], v, preferred_element_type=f32).astype(bf16)
    for s in range(groups):
        outs[s][...] = scratch[me ^ s]


def forward_z_kernel(*rest, groups, places):
    pieces = rest[:groups]
    outs, source = rest[groups:-1], rest[-1]
    me = lax.axis_index("zg")
    held = len(places)
    planes, rows, lanes = pieces[0].shape
    total = planes * groups
    for s in range(groups):
        source[me ^ s] = pieces[s][...]
    tile = min(16, rows)
    low = lax.broadcasted_iota(jnp.int32, (tile // 2, lanes), 1) < lanes // 2

    def step(n, carry):
        top = pl.multiple_of(n * tile, tile)

        def values():
            return [
                opened(source[z // planes, z % planes, pl.ds(top, tile), :].astype(f32), low) for z in range(total)
            ]

        def keep(k, v):
            chunk, place = places[k % held]
            outs[chunk][k // held, place, pl.ds(top, tile), :] = closed(v, low).astype(bf16)

        for k, v in enumerate(transform_list(values(), -1.0)):
            keep(2 * k, v)
        turned = [times(v, -2.0 * math.pi * z / (2 * total)) for z, v in enumerate(values())]
        for k, v in enumerate(transform_list(turned, -1.0)):
            keep(2 * k + 1, v)
        return carry

    lax.fori_loop(0, rows // tile, step, 0, unroll=2 if rows > tile else 1)


def inverse_z_kernel(*rest, groups, places, chunks):
    pieces = rest[:chunks]
    outs, target = rest[chunks:-1], rest[-1]
    me = lax.axis_index("zg")
    members, _, rows, lanes = pieces[0].shape
    held = len(places)
    total = members * held // 2
    planes = total // groups
    tile = min(16, rows)
    low = lax.broadcasted_iota(jnp.int32, (tile // 2, lanes), 1) < lanes // 2

    def step(n, carry):
        top = pl.multiple_of(n * tile, tile)

        def value(k):
            chunk, place = places[k % held]
            return opened(pieces[chunk][k // held, place, pl.ds(top, tile), :].astype(f32), low)

        even = transform_list([value(k) for k in range(0, 2 * total, 2)], 1.0)
        odd = transform_list([value(k) for k in range(1, 2 * total, 2)], 1.0)
        for z in range(total):
            v = plus(even[z], times(odd[z], 2.0 * math.pi * z / (2 * total)))
            target[z // planes, z % planes, pl.ds(top, tile), :] = closed(v, low).astype(bf16)
        return carry

    lax.fori_loop(0, rows // tile, step, 0, unroll=2 if rows > tile else 1)
    for s in range(groups):
        outs[s][...] = target[me ^ s]


def middle_kernel(
    scale_ref, tabley_hbm, forward_hbm, inverse_hbm, green_hbm, *rest, first, chunk, groups, members
):
    pieces = rest[:groups]
    outs = rest[groups : 2 * groups]
    tabley, forward, inverse, green, spread, wide, product, sems = rest[2 * groups :]
    me = lax.axis_index("zg")
    _, comps, rows, lanes = pieces[0].shape
    half = rows // 2
    g = pl.program_id(0)
    plane = first + g
    copies = [
        pltpu.make_async_copy(tabley_hbm.at[me, me ^ t], tabley.at[pl.ds(t * lanes, lanes)], sems.at[t])
        for t in range(groups)
    ]
    copies.append(pltpu.make_async_copy(forward_hbm, forward, sems.at[groups]))
    copies.append(pltpu.make_async_copy(inverse_hbm, inverse, sems.at[groups + 1]))
    load = pltpu.make_async_copy(green_hbm.at[:, :, plane], green, sems.at[groups + 2])
    load.start()

    @pl.when(g == 0)
    def _():
        for c in copies:
            c.start()
        for c in copies[:groups]:
            c.wait()

    wave = tabley.shape[1] // 2
    for s in range(members):
        block = jnp.concatenate(
            [pieces[t][s].reshape(comps * rows, lanes) for t in range(groups)], axis=1
        )
        result = jnp.dot(block, tabley[...], preferred_element_type=f32).astype(bf16)
        start = s * half
        for j in range(comps):
            for p in range(2):
                spread[j, p, pl.ds(start, half), :] = result[j * rows + p * half : j * rows + (p + 1) * half]
    @pl.when(g == 0)
    def _():
        copies[groups].wait()

    for j in range(comps):
        for p in range(2):
            wide[j, p] = jnp.dot(forward[p], spread[j, p], preferred_element_type=f32)
    load.wait()
    many = wide.shape[2] // 2
    tile = 32

    def step(n, carry):
        top = pl.multiple_of(n * tile, tile)
        spectra = []
        for j in range(comps):
            re, im = [], []
            for p in range(2):
                c = wide[j, p, pl.ds(top, tile), :]
                s = wide[j, p, pl.ds(many + top, tile), :]
                re.append(c[:, :wave] - s[:, wave:])
                im.append(s[:, :wave] + c[:, wave:])
            spectra.append(((re[0] + re[1], im[0] + im[1]), (re[0] - re[1], im[0] - im[1])))
        totals = []
        for h in range(2):
            weights = [
                tuple(
                    green[c, e, pl.ds(h * many + top, tile), :].astype(f32) * scale_ref[plane, e]
                    for c in range(2)
                )
                for e in range(2 * comps)
            ]
            out = []
            for i in range(comps):
                re = im = None
                for j in range(comps):
                    gr, gi = weights[pairing[i][j]]
                    xr, xi = spectra[j][h]
                    r, m = gr * xr - gi * xi, gr * xi + gi * xr
                    re, im = (r, m) if re is None else (re + r, im + m)
                out.append((re, im))
            totals.append(out)
        for i in range(comps):
            for p in range(2):
                for c in range(2):
                    a, b = totals[0][i][c], totals[1][i][c]
                    product[i, p, pl.ds(top, tile), c * wave : (c + 1) * wave] = (
                        a + b if p == 0 else a - b
                    ).astype(bf16)
        return carry

    lax.fori_loop(0, many // tile, step, 0)
    @pl.when(g == 0)
    def _():
        copies[groups + 1].wait()

    count = inverse.shape[1] // 2
    for i in range(comps):
        for p in range(2):
            both = jnp.dot(inverse[p], product[i, p], preferred_element_type=f32)
            c, s = both[:count], both[count:]
            re = c[:, :wave] - s[:, wave:]
            im = s[:, :wave] + c[:, wave:]
            back = jnp.concatenate([re.astype(bf16), im.astype(bf16)], axis=1)
            share = lax.dot_general(
                back, tabley[...], (((1,), (1,)), ((), ())), preferred_element_type=f32
            ).astype(bf16)
            for b in range(members):
                for t in range(groups):
                    outs[t][b, i, p * half : (p + 1) * half, :] = share[
                        b * half : (b + 1) * half, t * lanes : (t + 1) * lanes
                    ]


def result_kernel(field_ref, order_ref, *rest, groups, factor):
    pieces, out, scratch = rest[:groups], rest[groups], rest[groups + 1]
    me = lax.axis_index("zg")
    _, comps, planes, rows, many = field_ref.shape
    part = many // groups
    lanes = 2 * part
    for s in range(groups):
        scratch[me ^ s] = pieces[s][...]
    low = lax.broadcasted_iota(jnp.int32, (rows, lanes), 1) < part
    for z in range(planes):
        for i in range(comps):
            for b in range(groups // 2):
                first, second = [
                    lax.dot_general(
                        order_ref[...], scratch[2 * b + h, z, i], (((0,), (0,)), ((), ())),
                        preferred_element_type=f32,
                    )
                    for h in range(2)
                ]
                re = jnp.where(low, first, swapped(second))
                im = jnp.where(low, swapped(first), second)
                for c, v in enumerate((re, im)):
                    field = field_ref[c, i, z, :, b * lanes : (b + 1) * lanes].astype(f32)
                    out[c, i, z, :, b * lanes : (b + 1) * lanes] = (field - v * factor).astype(bf16)


def smem():
    return pl.BlockSpec(memory_space=pltpu.SMEM)


def vmem():
    return pl.BlockSpec(memory_space=pltpu.VMEM)


def hbm():
    return pl.BlockSpec(memory_space=pl.ANY)


def call(kernel, specs, shapes, scratch, flops, args, name, grid=(), out_spec=None):
    many = isinstance(shapes, list)
    return pl.pallas_call(
        kernel,
        grid=grid,
        in_specs=specs,
        out_specs=(out_spec if isinstance(out_spec, list) else [out_spec] * len(shapes)) if many else out_spec,
        out_shape=shapes,
        scratch_shapes=scratch,
        compiler_params=pltpu.CompilerParams(vmem_limit_bytes=56 * 1024 * 1024),
        cost_estimate=pl.CostEstimate(flops=int(flops), transcendentals=0, bytes_accessed=1 << 20),
        name=name,
    )(*args)


def chunk_sizes(held):
    edge = max(1, held // 2)
    return [edge] * (held // edge)


def on_device(dipole_field, material, alpha_table, green_spectrum, green_scale):
    groups, members = lax.axis_size("zg"), lax.axis_size("xy")
    _, comps, planes, rows, rows_y = dipole_field.shape
    length_y = 2 * rows_y
    rows_x = rows * members
    length_x = 2 * rows_x
    total_z = planes * groups
    length_z = 2 * total_z
    held = length_z // members
    part = rows_y // groups
    lanes = 2 * part
    wave = length_y // groups
    counts = alpha_table.shape[0]
    tabley = table_y(rows_y, length_y, groups)
    forward, inverse = tables_x(rows_x, length_x)
    order = parity_order(rows)

    def send(value, axis, size, distance):
        return lax.ppermute(value, axis, [(i, i ^ distance) for i in range(size)])

    def exchange(parts, axis):
        return [parts[0]] + [send(parts[s], axis, len(parts), s) for s in range(1, len(parts))]

    def shape(*dims):
        return jax.ShapeDtypeStruct(dims, bf16)

    plane_block = pl.BlockSpec((2, comps, None, rows, rows_y), lambda z: (0, 0, z, 0, 0))
    part_block = pl.BlockSpec((None, comps, rows, lanes), lambda z: (z, 0, 0, 0))
    blocks = material.shape[2]
    parts = call(
        functools.partial(moments_kernel, groups=groups, counts=counts),
        [smem(), plane_block, pl.BlockSpec((None, blocks, rows), lambda z: (z, 0, 0)), vmem()],
        [shape(planes, comps, rows, lanes)] * groups,
        [VMEM((groups, comps, rows, lanes), bf16)],
        5e9,
        (jnp.transpose(alpha_table, (2, 3, 1, 0)), dipole_field, jnp.transpose(material, (0, 2, 1)), order),
        "moments",
        grid=(planes,),
        out_spec=part_block,
    )
    parts = exchange(parts, "zg")
    sizes = chunk_sizes(held)
    chunks = len(sizes)
    places = [(c, n) for c, size in enumerate(sizes) for n in range(size)]
    fulls = [shape(members, size, comps, rows, lanes) for size in sizes]
    comp_block = pl.BlockSpec((planes, None, rows, lanes), lambda j: (0, j, 0, 0))
    chunk_blocks = [
        pl.BlockSpec((members, size, None, rows, lanes), lambda j: (0, 0, j, 0, 0)) for size in sizes
    ]
    pieces = call(
        functools.partial(forward_z_kernel, groups=groups, places=places),
        [comp_block] * groups,
        fulls,
        [VMEM((groups, planes, rows, lanes), bf16)],
        4e9,
        tuple(parts),
        "forward_z",
        grid=(comps,),
        out_spec=chunk_blocks,
    )
    block = pl.BlockSpec((members, None, comps, rows, lanes), lambda g: (0, g, 0, 0, 0))

    def after(value, *others):
        return lax.optimization_barrier((value, *others))[0] if others else value

    def across(value):
        return lax.all_to_all(value, "xy", 0, 0, tiled=True)

    def gather(value):
        have = {0: value}
        bit = groups // 2
        while bit:
            for t in sorted(have):
                have[t ^ bit] = send(have[t], "zg", groups, bit)
            bit //= 2
        return [have[t] for t in range(groups)]

    def middle(r, have):
        return call(
            functools.partial(
                middle_kernel, first=sum(sizes[:r]), chunk=sizes[r], groups=groups, members=members
            ),
            [smem(), hbm(), hbm(), hbm(), hbm()] + [block] * groups,
            [fulls[r]] * groups,
            [
                VMEM((groups * lanes, 2 * wave), bf16),
                VMEM(forward.shape, bf16),
                VMEM(inverse.shape, bf16),
                VMEM((2, 2 * comps, length_x, wave), bf16),
                VMEM((comps, 2, rows_x // 2, 2 * wave), bf16),
                VMEM((comps, 2, length_x, 2 * wave), f32),
                VMEM((comps, 2, length_x // 2, 2 * wave), bf16),
                pltpu.SemaphoreType.DMA((groups + 3,)),
            ],
            8e9 * sizes[r],
            (jnp.transpose(green_scale), tabley, forward, inverse, green_spectrum, *have),
            "middle",
            grid=(sizes[r],),
            out_spec=block,
        )

    def reduce(shares):
        shares = dict(enumerate(shares))
        bit = 1
        while bit < groups // 2:
            moved = {t: send(shares[t ^ bit], "zg", groups, bit) for t in shares if not t & bit}
            shares = {
                t: (shares[t].astype(f32) + moved[t].astype(f32)).astype(bf16) if t else (shares[t], moved[t])
                for t in moved
            }
            bit *= 2
        own, moved = shares[0]
        last = send(shares[bit], "zg", groups, bit)
        return (own.astype(f32) + moved.astype(f32) + last.astype(f32)).astype(bf16)

    arrived, shared, totals = [], [], []
    for r in range(chunks):
        value = after(pieces[r], *arrived[-1:])
        arrived.append(across(value))
    ready = []
    for r in range(chunks):
        have = gather(after(arrived[r], *(shared[r - 2][:1] if r >= 2 else [])))
        ready.append(have)
        if r + 1 < chunks:
            have = [after(have[0], arrived[r + 1])] + have[1:]
        shared.append(middle(r, have))
    returned = []
    for r in range(chunks):
        returned.append(across(after(reduce(shared[r]), *returned[-1:])))
    parts = call(
        functools.partial(inverse_z_kernel, groups=groups, places=places, chunks=chunks),
        chunk_blocks,
        [shape(planes, comps, rows, lanes)] * groups,
        [VMEM((groups, planes, rows, lanes), bf16)],
        4e9,
        tuple(returned),
        "inverse_z",
        grid=(comps,),
        out_spec=comp_block,
    )
    parts = exchange(parts, "zg")
    return call(
        functools.partial(result_kernel, groups=groups, factor=1.0 / float(length_x * length_y * length_z)),
        [vmem()] * (2 + groups),
        shape(*dipole_field.shape),
        [VMEM((groups, planes, comps, rows, lanes), bf16)],
        3e9,
        (dipole_field, order, *parts),
        "result",
        out_spec=vmem(),
    )


def solution(mesh):
    return jax.shard_map(
        on_device,
        mesh=mesh,
        in_specs=(
            P(None, None, "zg", "xy", None),
            P("zg", "xy", None),
            P(),
            P(None, None, "xy", None, "zg"),
            P(None, "xy"),
        ),
        out_specs=P(None, None, "zg", "xy", None),
        check_vma=False,
    )
```

```python
import functools
import math

import jax
import jax.numpy as jnp
import numpy as np
from jax import lax
from jax.experimental import pallas as pl
from jax.experimental.pallas import tpu as pltpu
from jax.sharding import PartitionSpec as P

pairing = ((0, 3, 4), (3, 1, 5), (4, 5, 2))

VMEM = pltpu.VMEM
f32 = jnp.float32
bf16 = jnp.bfloat16


def phase(rows, cols, length):
    return (np.outer(rows, cols) % length).astype(np.float64) * (2.0 * math.pi / length)


def table_y(rows_y, length_y, groups):
    ny, nk = rows_y // groups, length_y // groups
    out = np.zeros((groups, groups, 2 * ny, 2 * nk), np.float32)
    for a in range(groups):
        for b in range(groups):
            angle = phase(np.arange(ny) + b * ny, np.arange(nk) + a * nk, length_y)
            cosine, sine = np.cos(angle), -np.sin(angle)
            out[a, b, :ny, :nk] = cosine
            out[a, b, ny:, :nk] = -sine
            out[a, b, :ny, nk:] = sine
            out[a, b, ny:, nk:] = cosine
    return jnp.asarray(out, bf16)


def tables_x(rows_x, length_x):
    half, many = length_x // 2, rows_x // 2
    forward = np.zeros((2, 2 * half, many), np.float32)
    inverse = np.zeros((2, 2 * many, half), np.float32)
    for p in range(2):
        angle = phase(np.arange(half), 2 * np.arange(many) + p, length_x)
        forward[p, :half], forward[p, half:] = np.cos(angle), -np.sin(angle)
        inverse[p, :many], inverse[p, many:] = np.cos(angle).T, np.sin(angle).T
    return jnp.asarray(forward, bf16), jnp.asarray(inverse, bf16)


def parity_order(rows):
    out = np.zeros((rows, rows), np.float32)
    for p in range(2):
        for m in range(rows // 2):
            out[p * (rows // 2) + m, 2 * m + p] = 1.0
    return jnp.asarray(out, bf16)


def swapped(value):
    return pltpu.roll(value, value.shape[-1] // 2, 1)


def opened(value, low):
    half = value.shape[0] // 2
    a, b = value[:half], value[half:]
    return jnp.where(low, a, swapped(b)), jnp.where(low, swapped(a), b)


def closed(pair, low):
    re, im = pair
    return jnp.concatenate([jnp.where(low, re, swapped(im)), jnp.where(low, swapped(re), im)], axis=0)


def plus(a, b):
    return a[0] + b[0], a[1] + b[1]


def minus(a, b):
    return a[0] - b[0], a[1] - b[1]


def times(pair, angle):
    re, im = pair
    turn = round(angle / (math.pi / 2.0), 9) % 4
    if turn in (0, 1, 2, 3):
        return ((re, im), (-im, re), (-re, -im), (im, -re))[int(turn)]
    c, s = math.cos(angle), math.sin(angle)
    return re * c - im * s, re * s + im * c


def transform_list(values, sign):
    n = len(values)
    if n == 1:
        return values
    even = transform_list(values[0::2], sign)
    odd = transform_list(values[1::2], sign)
    odd = [times(v, sign * 2.0 * math.pi * k / n) for k, v in enumerate(odd)]
    return [plus(e, o) for e, o in zip(even, odd)] + [minus(e, o) for e, o in zip(even, odd)]


def moments_kernel(alpha_ref, field_ref, material_ref, order_ref, *rest, groups, counts):
    outs, scratch = rest[:groups], rest[groups]
    me = lax.axis_index("zg")
    _, comps, rows, many = field_ref.shape
    blocks = material_ref.shape[0]
    cols = many // blocks
    part = many // groups
    per = cols // part
    low = lax.broadcasted_iota(jnp.int32, (rows, 2 * part), 1) < part
    diagonal = lax.broadcasted_iota(jnp.int32, (rows, rows), 0) == lax.broadcasted_iota(jnp.int32, (rows, rows), 1)
    for b in range(blocks):
        along = jnp.broadcast_to(material_ref[b : b + 1, :].astype(f32), (rows, rows))
        mat = jnp.sum(jnp.where(diagonal, along, 0.0), axis=1, keepdims=True)
        mat = jnp.broadcast_to(mat, (rows, cols))
        masks = [mat == float(n) for n in range(1, counts)]

        def pick(c, i, j):
            value = jnp.full((rows, cols), alpha_ref[i, j, c, 0], f32)
            for n in range(1, counts):
                value = jnp.where(masks[n - 1], alpha_ref[i, j, c, n], value)
            return value

        reals = [field_ref[0, j, :, b * cols : (b + 1) * cols].astype(f32) for j in range(comps)]
        imags = [field_ref[1, j, :, b * cols : (b + 1) * cols].astype(f32) for j in range(comps)]
        for i in range(comps):
            re = im = None
            for j in range(comps):
                ar, ai = pick(0, i, j), pick(1, i, j)
                r = ar * reals[j] - ai * imags[j]
                m = ar * imags[j] + ai * reals[j]
                re, im = (r, m) if re is None else (re + r, im + m)
            first = jnp.where(low, re, swapped(im)).astype(bf16)
            second = jnp.where(low, swapped(re), im).astype(bf16)
            for h, v in enumerate((first, second)):
                scratch[per * b + h, i] = jnp.dot(order_ref[...], v, preferred_element_type=f32).astype(bf16)
    for s in range(groups):
        outs[s][...] = scratch[me ^ s]


def forward_z_kernel(*rest, groups, places):
    pieces = rest[:groups]
    outs, source = rest[groups:-1], rest[-1]
    me = lax.axis_index("zg")
    held = len(places)
    planes, rows, lanes = pieces[0].shape
    total = planes * groups
    for s in range(groups):
        source[me ^ s] = pieces[s][...]
    tile = min(16, rows)
    low = lax.broadcasted_iota(jnp.int32, (tile // 2, lanes), 1) < lanes // 2

    def step(n, carry):
        top = pl.multiple_of(n * tile, tile)

        def values():
            return [
                opened(source[z // planes, z % planes, pl.ds(top, tile), :].astype(f32), low) for z in range(total)
            ]

        def keep(k, v):
            chunk, place = places[k % held]
            outs[chunk][k // held, place, pl.ds(top, tile), :] = closed(v, low).astype(bf16)

        for k, v in enumerate(transform_list(values(), -1.0)):
            keep(2 * k, v)
        turned = [times(v, -2.0 * math.pi * z / (2 * total)) for z, v in enumerate(values())]
        for k, v in enumerate(transform_list(turned, -1.0)):
            keep(2 * k + 1, v)
        return carry

    lax.fori_loop(0, rows // tile, step, 0, unroll=2 if rows > tile else 1)


def inverse_z_kernel(*rest, groups, places, chunks):
    pieces = rest[:chunks]
    outs, target = rest[chunks:-1], rest[-1]
    me = lax.axis_index("zg")
    members, _, rows, lanes = pieces[0].shape
    held = len(places)
    total = members * held // 2
    planes = total // groups
    tile = min(16, rows)
    low = lax.broadcasted_iota(jnp.int32, (tile // 2, lanes), 1) < lanes // 2

    def step(n, carry):
        top = pl.multiple_of(n * tile, tile)

        def value(k):
            chunk, place = places[k % held]
            return opened(pieces[chunk][k // held, place, pl.ds(top, tile), :].astype(f32), low)

        even = transform_list([value(k) for k in range(0, 2 * total, 2)], 1.0)
        odd = transform_list([value(k) for k in range(1, 2 * total, 2)], 1.0)
        for z in range(total):
            v = plus(even[z], times(odd[z], 2.0 * math.pi * z / (2 * total)))
            target[z // planes, z % planes, pl.ds(top, tile), :] = closed(v, low).astype(bf16)
        return carry

    lax.fori_loop(0, rows // tile, step, 0, unroll=2 if rows > tile else 1)
    for s in range(groups):
        outs[s][...] = target[me ^ s]


def middle_kernel(
    scale_ref, tabley_hbm, forward_hbm, inverse_hbm, green_hbm, *rest, first, chunk, groups, members
):
    pieces = rest[:groups]
    outs = rest[groups : 2 * groups]
    tabley, forward, inverse, green, spread, wide, product, sems = rest[2 * groups :]
    me = lax.axis_index("zg")
    _, comps, rows, lanes = pieces[0].shape
    half = rows // 2
    g = pl.program_id(0)
    plane = first + g
    copies = [
        pltpu.make_async_copy(tabley_hbm.at[me, me ^ t], tabley.at[pl.ds(t * lanes, lanes)], sems.at[t])
        for t in range(groups)
    ]
    copies.append(pltpu.make_async_copy(forward_hbm, forward, sems.at[groups]))
    copies.append(pltpu.make_async_copy(inverse_hbm, inverse, sems.at[groups + 1]))
    load = pltpu.make_async_copy(green_hbm.at[:, :, plane], green, sems.at[groups + 2])

    @pl.when(g == 0)
    def _():
        for c in copies:
            c.start()

    load.start()

    @pl.when(g == 0)
    def _():
        for c in copies[:groups]:
            c.wait()

    wave = tabley.shape[1] // 2
    for s in range(members):
        block = jnp.concatenate(
            [pieces[t][s].reshape(comps * rows, lanes) for t in range(groups)], axis=1
        )
        result = jnp.dot(block, tabley[...], preferred_element_type=f32).astype(bf16)
        start = s * half
        for j in range(comps):
            for p in range(2):
                spread[j, p, pl.ds(start, half), :] = result[j * rows + p * half : j * rows + (p + 1) * half]
    @pl.when(g == 0)
    def _():
        copies[groups].wait()

    for j in range(comps):
        for p in range(2):
            wide[j, p] = jnp.dot(forward[p], spread[j, p], preferred_element_type=f32)
    load.wait()
    many = wide.shape[2] // 2
    tile = 32

    def step(n, carry):
        top = pl.multiple_of(n * tile, tile)
        spectra = []
        for j in range(comps):
            re, im = [], []
            for p in range(2):
                c = wide[j, p, pl.ds(top, tile), :]
                s = wide[j, p, pl.ds(many + top, tile), :]
                re.append(c[:, :wave] - s[:, wave:])
                im.append(s[:, :wave] + c[:, wave:])
            spectra.append(((re[0] + re[1], im[0] + im[1]), (re[0] - re[1], im[0] - im[1])))
        totals = []
        for h in range(2):
            weights = [
                tuple(
                    green[c, e, pl.ds(h * many + top, tile), :].astype(f32) * scale_ref[plane, e]
                    for c in range(2)
                )
                for e in range(2 * comps)
            ]
            out = []
            for i in range(comps):
                re = im = None
                for j in range(comps):
                    gr, gi = weights[pairing[i][j]]
                    xr, xi = spectra[j][h]
                    r, m = gr * xr - gi * xi, gr * xi + gi * xr
                    re, im = (r, m) if re is None else (re + r, im + m)
                out.append((re, im))
            totals.append(out)
        for i in range(comps):
            for p in range(2):
                for c in range(2):
                    a, b = totals[0][i][c], totals[1][i][c]
                    product[i, p, pl.ds(top, tile), c * wave : (c + 1) * wave] = (
                        a + b if p == 0 else a - b
                    ).astype(bf16)
        return carry

    lax.fori_loop(0, many // tile, step, 0)
    @pl.when(g == 0)
    def _():
        copies[groups + 1].wait()

    count = inverse.shape[1] // 2
    for i in range(comps):
        for p in range(2):
            both = jnp.dot(inverse[p], product[i, p], preferred_element_type=f32)
            c, s = both[:count], both[count:]
            re = c[:, :wave] - s[:, wave:]
            im = s[:, :wave] + c[:, wave:]
            back = jnp.concatenate([re.astype(bf16), im.astype(bf16)], axis=1)
            share = lax.dot_general(
                back, tabley[...], (((1,), (1,)), ((), ())), preferred_element_type=f32
            ).astype(bf16)
            for b in range(members):
                for t in range(groups):
                    outs[t][b, i, p * half : (p + 1) * half, :] = share[
                        b * half : (b + 1) * half, t * lanes : (t + 1) * lanes
                    ]


def result_kernel(field_ref, order_ref, *rest, groups, factor):
    pieces, out, scratch = rest[:groups], rest[groups], rest[groups + 1]
    me = lax.axis_index("zg")
    _, comps, planes, rows, many = field_ref.shape
    part = many // groups
    lanes = 2 * part
    for s in range(groups):
        scratch[me ^ s] = pieces[s][...]
    low = lax.broadcasted_iota(jnp.int32, (rows, lanes), 1) < part
    for z in range(planes):
        for i in range(comps):
            for b in range(groups // 2):
                first, second = [
                    lax.dot_general(
                        order_ref[...], scratch[2 * b + h, z, i], (((0,), (0,)), ((), ())),
                        preferred_element_type=f32,
                    )
                    for h in range(2)
                ]
                re = jnp.where(low, first, swapped(second))
                im = jnp.where(low, swapped(first), second)
                for c, v in enumerate((re, im)):
                    field = field_ref[c, i, z, :, b * lanes : (b + 1) * lanes].astype(f32)
                    out[c, i, z, :, b * lanes : (b + 1) * lanes] = (field - v * factor).astype(bf16)


def smem():
    return pl.BlockSpec(memory_space=pltpu.SMEM)


def vmem():
    return pl.BlockSpec(memory_space=pltpu.VMEM)


def hbm():
    return pl.BlockSpec(memory_space=pl.ANY)


def call(kernel, specs, shapes, scratch, flops, args, name, grid=(), out_spec=None):
    many = isinstance(shapes, list)
    return pl.pallas_call(
        kernel,
        grid=grid,
        in_specs=specs,
        out_specs=(out_spec if isinstance(out_spec, list) else [out_spec] * len(shapes)) if many else out_spec,
        out_shape=shapes,
        scratch_shapes=scratch,
        compiler_params=pltpu.CompilerParams(vmem_limit_bytes=56 * 1024 * 1024),
        cost_estimate=pl.CostEstimate(flops=int(flops), transcendentals=0, bytes_accessed=1 << 20),
        name=name,
    )(*args)


def chunk_sizes(held):
    edge = max(1, held // 2)
    return [edge] * (held // edge)


def on_device(dipole_field, material, alpha_table, green_spectrum, green_scale):
    groups, members = lax.axis_size("zg"), lax.axis_size("xy")
    _, comps, planes, rows, rows_y = dipole_field.shape
    length_y = 2 * rows_y
    rows_x = rows * members
    length_x = 2 * rows_x
    total_z = planes * groups
    length_z = 2 * total_z
    held = length_z // members
    part = rows_y // groups
    lanes = 2 * part
    wave = length_y // groups
    counts = alpha_table.shape[0]
    tabley = table_y(rows_y, length_y, groups)
    forward, inverse = tables_x(rows_x, length_x)
    order = parity_order(rows)

    def send(value, axis, size, distance):
        return lax.ppermute(value, axis, [(i, i ^ distance) for i in range(size)])

    def exchange(parts, axis):
        return [parts[0]] + [send(parts[s], axis, len(parts), s) for s in range(1, len(parts))]

    def shape(*dims):
        return jax.ShapeDtypeStruct(dims, bf16)

    plane_block = pl.BlockSpec((2, comps, None, rows, rows_y), lambda z: (0, 0, z, 0, 0))
    part_block = pl.BlockSpec((None, comps, rows, lanes), lambda z: (z, 0, 0, 0))
    blocks = material.shape[2]
    parts = call(
        functools.partial(moments_kernel, groups=groups, counts=counts),
        [smem(), plane_block, pl.BlockSpec((None, blocks, rows), lambda z: (z, 0, 0)), vmem()],
        [shape(planes, comps, rows, lanes)] * groups,
        [VMEM((groups, comps, rows, lanes), bf16)],
        5e9,
        (jnp.transpose(alpha_table, (2, 3, 1, 0)), dipole_field, jnp.transpose(material, (0, 2, 1)), order),
        "moments",
        grid=(planes,),
        out_spec=part_block,
    )
    parts = exchange(parts, "zg")
    sizes = chunk_sizes(held)
    chunks = len(sizes)
    places = [(c, n) for c, size in enumerate(sizes) for n in range(size)]
    fulls = [shape(members, size, comps, rows, lanes) for size in sizes]
    comp_block = pl.BlockSpec((planes, None, rows, lanes), lambda j: (0, j, 0, 0))
    chunk_blocks = [
        pl.BlockSpec((members, size, None, rows, lanes), lambda j: (0, 0, j, 0, 0)) for size in sizes
    ]
    pieces = call(
        functools.partial(forward_z_kernel, groups=groups, places=places),
        [comp_block] * groups,
        fulls,
        [VMEM((groups, planes, rows, lanes), bf16)],
        4e9,
        tuple(parts),
        "forward_z",
        grid=(comps,),
        out_spec=chunk_blocks,
    )
    block = pl.BlockSpec((members, None, comps, rows, lanes), lambda g: (0, g, 0, 0, 0))

    def after(value, *others):
        return lax.optimization_barrier((value, *others))[0] if others else value

    def across(value):
        return lax.all_to_all(value, "xy", 0, 0, tiled=True)

    def gather(value):
        have = {0: value}
        bit = groups // 2
        while bit:
            for t in sorted(have):
                have[t ^ bit] = send(have[t], "zg", groups, bit)
            bit //= 2
        return [have[t] for t in range(groups)]

    def middle(r, have):
        return call(
            functools.partial(
                middle_kernel, first=sum(sizes[:r]), chunk=sizes[r], groups=groups, members=members
            ),
            [smem(), hbm(), hbm(), hbm(), hbm()] + [block] * groups,
            [fulls[r]] * groups,
            [
                VMEM((groups * lanes, 2 * wave), bf16),
                VMEM(forward.shape, bf16),
                VMEM(inverse.shape, bf16),
                VMEM((2, 2 * comps, length_x, wave), bf16),
                VMEM((comps, 2, rows_x // 2, 2 * wave), bf16),
                VMEM((comps, 2, length_x, 2 * wave), f32),
                VMEM((comps, 2, length_x // 2, 2 * wave), bf16),
                pltpu.SemaphoreType.DMA((groups + 3,)),
            ],
            8e9 * sizes[r],
            (jnp.transpose(green_scale), tabley, forward, inverse, green_spectrum, *have),
            "middle",
            grid=(sizes[r],),
            out_spec=block,
        )

    def reduce(shares):
        shares = dict(enumerate(shares))
        bit = 1
        while bit < groups // 2:
            moved = {t: send(shares[t ^ bit], "zg", groups, bit) for t in shares if not t & bit}
            shares = {
                t: (shares[t].astype(f32) + moved[t].astype(f32)).astype(bf16) if t else (shares[t], moved[t])
                for t in moved
            }
            bit *= 2
        own, moved = shares[0]
        last = send(shares[bit], "zg", groups, bit)
        return (own.astype(f32) + moved.astype(f32) + last.astype(f32)).astype(bf16)

    arrived, shared, totals = [], [], []
    for r in range(chunks):
        value = after(pieces[r], *arrived[-1:])
        arrived.append(across(value))
    ready = []
    for r in range(chunks):
        have = gather(after(arrived[r], *(shared[r - 2][:1] if r >= 2 else [])))
        ready.append(have)
        if r + 1 < chunks:
            have = [after(have[0], arrived[r + 1])] + have[1:]
        shared.append(middle(r, have))
    returned = []
    for r in range(chunks):
        returned.append(across(after(reduce(shared[r]), *returned[-1:])))
    parts = call(
        functools.partial(inverse_z_kernel, groups=groups, places=places, chunks=chunks),
        chunk_blocks,
        [shape(planes, comps, rows, lanes)] * groups,
        [VMEM((groups, planes, rows, lanes), bf16)],
        4e9,
        tuple(returned),
        "inverse_z",
        grid=(comps,),
        out_spec=comp_block,
    )
    parts = exchange(parts, "zg")
    return call(
        functools.partial(result_kernel, groups=groups, factor=1.0 / float(length_x * length_y * length_z)),
        [vmem()] * (2 + groups),
        shape(*dipole_field.shape),
        [VMEM((groups, planes, comps, rows, lanes), bf16)],
        3e9,
        (dipole_field, order, *parts),
        "result",
        out_spec=vmem(),
    )


def solution(mesh):
    return jax.shard_map(
        on_device,
        mesh=mesh,
        in_specs=(
            P(None, None, "zg", "xy", None),
            P("zg", "xy", None),
            P(),
            P(None, None, "xy", None, "zg"),
            P(None, "xy"),
        ),
        out_specs=P(None, None, "zg", "xy", None),
        check_vma=False,
    )
```
